512 devices in a mesh: scen: 2 (over y), row: 32 (over z), col: 4 (over x), layer: 2 (over core).
Axes of the slice: x: 4, y: 2, z: 32, core: 2. Of those that a mesh axis runs over, the one named last changes fastest.
The devices are a block of a 4x8x32 slice.
Arguments:
- current: float32 [2, 8192, 4096], P('layer', ('scen', 'row'), 'col'), parts along dimension 1, may hold values from 0.5 to 10
- node_class: int32 [2, 8192, 4096], P('layer', ('scen', 'row'), 'col'), parts along dimension 1, may hold values from 0 to 7
- class_conductance: float32 [2, 8], P('layer'), may hold values from 0.5 to 4
- pad_mask: int32 [2, 8192, 4096], P('layer', ('scen', 'row'), 'col'), parts along dimension 1, may hold values 0 or 1
- via_mask: int32 [8192, 4096], P(('scen', 'row'), 'col'), parts along dimension 0, may hold values 0 or 1
Outputs:
- drop: float32 [2, 8192, 4096], P('layer', ('scen', 'row'), 'col'), parts along dimension 1
- residual: float32 [2, 8192, 4096], P('layer', ('scen', 'row'), 'col'), parts along dimension 1
- worst: float32 [2, 8192, 4096], P('layer', ('scen', 'row'), 'col'), parts along dimension 1
The draws below stay inside these ranges and needn't reach their ends.
There are 2 independent parts, one for each index of `scen`. The reference program is written for one: setup_inputs(seed, part) draws one part's arguments, and reference() takes and returns one part's arrays. A program takes and returns all parts, laid end to end along the dimension named above; an argument that names none is the same for every part. Nothing has to cross between parts.
All inputs are finite; a program needn't handle non-finite values. No bound on the sum of `pad_mask` or of `via_mask` on one device may be relied on, other than what follows from the above.
Results may differ from the reference program's by a relative error of at most 0.0003.
Values sent between devices are 32-bit elements; how exact they have to be, the bound alone decides.
A program may use at most 64 MiB of HBM per device.

```python
import math
import jax
import jax.numpy as jnp

CLASSES = 8
ITERS = 2
NX = 4096
NY = 4096
LAYERS = 2


def with_ends(entries, stream_key, smallest, high):
    spot = [jax.random.randint(jax.random.fold_in(stream_key, axis), (), 0, length) for axis, length in enumerate(entries.shape)]
    longest = entries.shape.index(max(entries.shape))
    next_to = spot[:longest] + [(spot[longest] + 1) % entries.shape[longest]] + spot[longest + 1:]
    return entries.at[tuple(spot)].set(smallest).at[tuple(next_to)].set(high)


def shard_levels(rng, shape, shards, low, high):
    def one(position, shards_of):
        steps = jax.random.uniform(jax.random.fold_in(jax.random.fold_in(rng, 6), position), (shards_of,), jnp.float32, low / len(shards), high / len(shards))
        return jnp.repeat(jnp.exp(steps), shape[position] // shards_of).reshape((-1,) + (1,) * (len(shape) - position - 1))

    gain = one(*shards[0])
    for cut in shards[1:]:
        gain = gain * one(*cut)
    return gain


def setup_inputs(seed: int = 0, part: int = 0) -> dict:
    streams_of = jax.random.split(jax.random.key(seed), 6)
    own_keys = jax.random.split(jax.random.fold_in(streams_of[5], part), 6)
    return {
        "current": jnp.clip(jnp.exp(math.log(10.0) - 2.9957323 * jax.random.uniform(own_keys[0], (LAYERS, NX, NY), jnp.float32) ** shard_levels(own_keys[0], (LAYERS, NX, NY), ((0, 2), (1, 32), (2, 4)), -0.2, 0.2)), 0.5, 10.0),
        "node_class": with_ends(jax.random.randint(own_keys[1], (LAYERS, NX, NY), 0, CLASSES), jax.random.fold_in(own_keys[1], 1), 0, CLASSES - 1).astype(jnp.int32),
        "class_conductance": jnp.clip(jnp.exp(math.log(4.0) - 2.0794415 * jax.random.uniform(streams_of[2], (LAYERS, CLASSES), jnp.float32) ** shard_levels(streams_of[2], (LAYERS, CLASSES), ((0, 2),), -0.2, 0.2)), 0.5, 4.0),
        "pad_mask": with_ends((jax.random.randint(own_keys[3], (LAYERS, NX, NY), 0, 16) < 1).astype(jnp.int32), jax.random.fold_in(own_keys[3], 1), 0, 1),
        "via_mask": with_ends((jax.random.randint(own_keys[4], (NX, NY), 0, 2) < 1).astype(jnp.int32), jax.random.fold_in(own_keys[4], 1), 0, 1),
    }


via_conductance = 2.0
pad_conductance = 4.0
leakage = 0.05


def lookup(node_class, class_conductance):
    cond = jnp.zeros(node_class.shape, jnp.float32)
    for klass in range(class_conductance.shape[1]):
        cond = cond + jnp.where(node_class == klass, class_conductance[:, klass][:, None, None], jnp.float32(0.0))
    return cond


def edge_terms(cond):
    padded = jnp.pad(cond, ((0, 0), (1, 1), (1, 1)))
    beside_all = (padded[:, :-2, 1:-1], padded[:, 2:, 1:-1], padded[:, 1:-1, :-2], padded[:, 1:-1, 2:])
    return tuple(jnp.where(other > 0.0, 0.5 * (cond + other), jnp.float32(0.0)) for other in beside_all)


def apply_grid(values, edges, diagonal, coupling):
    padded = jnp.pad(values, ((0, 0), (1, 1), (1, 1)))
    beside = edges[0] * padded[:, :-2, 1:-1] + edges[1] * padded[:, 2:, 1:-1]
    beside = beside + edges[2] * padded[:, 1:-1, :-2] + edges[3] * padded[:, 1:-1, 2:]
    return diagonal * values - beside - coupling * values[::-1]


def reference(current, node_class, class_conductance, pad_mask, via_mask):
    cond = lookup(node_class, class_conductance)
    edges = edge_terms(cond)
    coupling = via_conductance * via_mask.astype(jnp.float32)
    diagonal = edges[0] + edges[1] + edges[2] + edges[3] + coupling + pad_conductance * pad_mask.astype(jnp.float32) + leakage
    drop_field = jnp.zeros_like(current)
    resid = current
    precond = resid / diagonal
    direction = precond
    energy_now = jnp.sum(resid * precond)
    worst_field = drop_field
    for iteration in range(ITERS):
        image = apply_grid(direction, edges, diagonal, coupling)
        step_size = energy_now / jnp.sum(direction * image)
        drop_field = drop_field + step_size * direction
        resid = resid - step_size * image
        worst_field = drop_field if iteration == 0 else jnp.maximum(worst_field, drop_field)
        if iteration + 1 < ITERS:
            precond = resid / diagonal
            energy_next = jnp.sum(resid * precond)
            direction = precond + (energy_next / energy_now) * direction
            energy_now = energy_next
    return drop_field, resid, worst_field
```

```python
import functools

import jax
import jax.numpy as jnp
from jax import lax
from jax.sharding import PartitionSpec as P


via_conductance = 2.0
pad_conductance = 4.0
leakage = 0.05


def with_halo(value, sides, width):
    edges = {}
    for axis, dim in sides:
        size, length = (lax.axis_size(axis), value.shape[dim])
        up = [(i, (i + 1) % size) for i in range(size - 1)]
        last = lax.slice_in_dim(value, length - width, length, axis=dim)
        initial = lax.slice_in_dim(value, 0, width, axis=dim)
        edges[dim] = (
            lax.ppermute(last, axis, up),
            lax.ppermute(initial, axis, [(b, a) for a, b in up]),
        )
    done = []
    for _, dim in sides:
        low, high = edges[dim]
        around = [(width, width) if d in done else (0, 0) for d in range(value.ndim)]
        value = jnp.concatenate([jnp.pad(low, around), value, jnp.pad(high, around)], axis=dim)
        done.append(dim)
    return value


def from_partner(value, axis, stride):
    return lax.ppermute(value, axis, [(i, i ^ 1 << stride) for i in range(lax.axis_size(axis))])


def over_axes(value, axes):
    return functools.reduce(lax.psum, axes, value)


def lookup(node_class, class_conductance):
    cond = jnp.zeros(node_class.shape, jnp.float32)
    for klass in range(class_conductance.shape[1]):
        cond = cond + jnp.where(
            node_class == klass, class_conductance[:, klass][:, None, None], jnp.float32(0.0)
        )
    return cond


def edge_terms(cond):
    padded = with_halo(cond, (("row", 1), ("col", 2)), 1)
    beside_all = (
        padded[:, :-2, 1:-1],
        padded[:, 2:, 1:-1],
        padded[:, 1:-1, :-2],
        padded[:, 1:-1, 2:],
    )
    return tuple(
        (jnp.where(other > 0.0, 0.5 * (cond + other), jnp.float32(0.0)) for other in beside_all)
    )


def apply_grid(values, edges, diagonal, coupling):
    padded = with_halo(values, (("row", 1), ("col", 2)), 1)
    partner = from_partner(values, "layer", 0)
    beside = edges[0] * padded[:, :-2, 1:-1] + edges[1] * padded[:, 2:, 1:-1]
    beside = beside + edges[2] * padded[:, 1:-1, :-2] + edges[3] * padded[:, 1:-1, 2:]
    return diagonal * values - beside - coupling * partner


def local(current, node_class, class_conductance, pad_mask, via_mask):
    cond = lookup(node_class, class_conductance)
    edges = edge_terms(cond)
    coupling = via_conductance * via_mask.astype(jnp.float32)
    diagonal = (
        edges[0]
        + edges[1]
        + edges[2]
        + edges[3]
        + coupling
        + pad_conductance * pad_mask.astype(jnp.float32)
        + leakage
    )
    precond = current / diagonal
    image = apply_grid(precond, edges, diagonal, coupling)
    second = image / diagonal
    second_image = apply_grid(second, edges, diagonal, coupling)
    sums = jnp.stack(
        [
            jnp.sum(current * precond),
            jnp.sum(precond * image),
            jnp.sum(image * second),
            jnp.sum(second * second_image),
        ]
    )
    sums = over_axes(sums, ("layer", "col", "row"))
    first_step = sums[0] / sums[1]
    ratio = sums[0] * sums[2] / (sums[1] * sums[1]) - 1.0
    energy = ratio * sums[0]
    grown = 1.0 + ratio
    curve = grown * grown * sums[1] - 2.0 * first_step * grown * sums[2]
    curve = curve + first_step * first_step * sums[3]
    second_step = energy / curve
    along = first_step + second_step * grown
    back = first_step * second_step
    drop_field = along * precond - back * second
    resid = current - along * image + back * second_image
    worst_field = jnp.maximum(first_step * precond, drop_field)
    return (drop_field, resid, worst_field)


def solution(mesh):
    in_specs = (
        P("layer", ("scen", "row"), "col"),
        P("layer", ("scen", "row"), "col"),
        P("layer", None),
        P("layer", ("scen", "row"), "col"),
        P(("scen", "row"), "col"),
    )
    out_specs = (
        P("layer", ("scen", "row"), "col"),
        P("layer", ("scen", "row"), "col"),
        P("layer", ("scen", "row"), "col"),
    )
    return jax.shard_map(local, mesh=mesh, in_specs=in_specs, out_specs=out_specs, check_vma=False)
```

```python
import functools

import jax
import jax.numpy as jnp
from jax import lax
from jax.experimental import pallas as pl
from jax.experimental.pallas import tpu as pltpu
from jax.sharding import PartitionSpec as P

MESH = pl.DeviceIdType.MESH

via_conductance = 2.0
pad_conductance = 4.0
leakage = 0.05

S0, S1, Q0, Q1, Q2, E0, E1, E2, GUESS = range(9)


def lanes_of(shape):
    return lax.broadcasted_iota(jnp.int32, shape, len(shape) - 1)


def rows_of(shape):
    return lax.broadcasted_iota(jnp.int32, shape, len(shape) - 2)


def pick(record, lane, axis=None):
    kept = jnp.where(lanes_of(record.shape) == lane, record, 0.0)
    return jnp.sum(kept, axis=axis, keepdims=True)


def by_lane(shape, entries):
    lane = lanes_of(shape)
    out = jnp.zeros(shape, jnp.float32)
    for where, value in entries:
        out = jnp.where(lane == where, value, out)
    return out


def fold(value):
    parts = [value[:, i : i + 128] for i in range(0, value.shape[1], 128)]
    while len(parts) > 1:
        parts = [a + b for a, b in zip(parts[::2], parts[1::2])]
    return parts[0]


def kernel(
    nz,
    nx,
    nc,
    cur_hbm,
    cls_hbm,
    cc_ref,
    pad_hbm,
    via_hbm,
    z_hbm,
    w_hbm,
    y_hbm,
    u_hbm,
    scal_ref,
    cur,
    cls,
    pad,
    via,
    cond_p,
    z_p,
    y_p,
    inv,
    w,
    u,
    zother,
    yother,
    srow,
    scol,
    rrow,
    rcol,
    srec,
    plane,
    zrec,
    zbuf,
    in_sem,
    out_sem,
    halo_ssem,
    halo_rsem,
    other_ssem,
    other_rsem,
    plane_ssem,
    plane_rsem,
    z_ssem,
    z_rsem,
    ready,
):
    iz, ix, ic = lax.axis_index("row"), lax.axis_index("col"), lax.axis_index("layer")
    rows, cols = cur.shape
    chunks = rows // 8
    np_ = nx * nc
    me = ix * nc + ic

    loads = [
        pltpu.make_async_copy(src, dst, in_sem.at[i])
        for i, (src, dst) in enumerate(
            ((cls_hbm, cls), (cur_hbm, cur), (pad_hbm, pad), (via_hbm, via))
        )
    ]
    for copy in loads:
        copy.start()

    rrow[...] = jnp.zeros(rrow.shape, jnp.float32)
    rcol[...] = jnp.zeros(rcol.shape, jnp.float32)

    barrier = pltpu.get_barrier_semaphore()
    zup, zdown = lax.rem(iz + nz - 1, nz), lax.rem(iz + 1, nz)
    for near in (zup, zdown):
        pl.semaphore_signal(barrier, inc=1, device_id={"row": near}, device_id_type=MESH)

    def plane_peer(step):
        other = lax.rem(me + step, np_)
        return {"col": other // nc, "layer": lax.rem(other, nc)}

    for step in range(1, np_):
        pl.semaphore_signal(barrier, inc=1, device_id=plane_peer(step), device_id_type=MESH)
    pl.semaphore_wait(barrier, np_ + 1)

    levels = (nz // 2).bit_length() - 1

    def greet(level):
        if level >= levels:
            return
        far = 1 << level
        for near in (lax.rem(iz + far, nz), lax.rem(iz + nz - far, nz)):
            pl.semaphore_signal(
                ready.at[level], inc=1, device_id={"row": near}, device_id_type=MESH
            )

    def greeted(level):
        if level < levels:
            pl.semaphore_wait(ready.at[level], 2)

    greet(0)

    sides = (
        (srow, rrow, 0, 1, iz > 0, iz < nz - 1, {"row": iz - 1}),
        (srow, rrow, 1, 0, iz < nz - 1, iz > 0, {"row": iz + 1}),
        (scol, rcol, 0, 1, ix > 0, ix < nx - 1, {"col": ix - 1}),
        (scol, rcol, 1, 0, ix < nx - 1, ix > 0, {"col": ix + 1}),
    )

    def halo(turn, i):
        src, dst, mine, theirs, _, _, target = sides[i]
        return pltpu.make_async_remote_copy(
            src_ref=src.at[turn, mine],
            dst_ref=dst.at[turn, theirs],
            send_sem=halo_ssem.at[turn, i],
            recv_sem=halo_rsem.at[turn, i],
            device_id=target,
            device_id_type=MESH,
        )

    def send_halo(turn, field, left, right):
        srow[turn, 0] = field[8:9, :]
        srow[turn, 1] = field[rows + 7 : rows + 8, :]
        scol[turn, 0] = left
        scol[turn, 1] = right
        for i in range(4):
            pl.when(sides[i][4])(halo(turn, i).start)

    def take_halo(turn, field):
        for i in range(4):
            pl.when(sides[i][5])(halo(turn, i).wait_recv)
        field[0:8, :] = jnp.broadcast_to(rrow[turn, 0], (8, cols))
        field[rows + 8 : rows + 16, :] = jnp.broadcast_to(rrow[turn, 1], (8, cols))

    def end_halo(turn):
        for i in range(4):
            pl.when(sides[i][4])(halo(turn, i).wait_send)

    def to_other(turn, src, dst):
        return pltpu.make_async_remote_copy(
            src_ref=src.at[pl.ds(8, rows)],
            dst_ref=dst,
            send_sem=other_ssem.at[turn],
            recv_sem=other_rsem.at[turn],
            device_id={"layer": 1 - ic},
            device_id_type=MESH,
        )

    tile = (8, cols)
    block = (8, 128)
    zero = jnp.zeros(block, jnp.float32)
    sub = rows_of(tile)
    narrow_lane = lanes_of(block)

    def at(k, shift=0):
        return pl.ds(pl.multiple_of(8 * k + shift, 8), 8)

    def packed(k, value, left, right):
        here = narrow_lane == k
        left = jnp.where(here, pltpu.roll(value[:, :128], k, 1), left)
        right = jnp.where(here, pltpu.roll(value[:, cols - 128 :], k + 1, 1), right)
        return left, right

    def around(k, prev, here, after, left, right):
        up = pltpu.roll(jnp.where(sub == 7, prev, here), 1, 0)
        down = pltpu.roll(jnp.where(sub == 0, after, here), 7, 0)
        left = pltpu.roll(left, lax.rem(128 - k, 128), 1)
        right = pltpu.roll(right, 127 - k, 1)
        west = pltpu.roll(here, 1, 1)
        west = jnp.concatenate(
            [jnp.where(narrow_lane == 0, left, west[:, :128]), west[:, 128:]], axis=1
        )
        east = pltpu.roll(here, cols - 1, 1)
        east = jnp.concatenate(
            [
                east[:, : cols - 128],
                jnp.where(narrow_lane == 127, right, east[:, cols - 128 :]),
            ],
            axis=1,
        )
        return (up + down) + (west + east)

    loads[0].wait()

    def look_up(k, carry):
        klass = cls[at(k), :]
        level = [cc_ref[0, i] for i in range(8)]
        for bit in range(3):
            high = (klass & (1 << bit)) != 0
            level = [jnp.where(high, b, a) for a, b in zip(level[::2], level[1::2])]
        cond_p[at(k, 8), :] = level[0]
        return packed(k, level[0], *carry)

    left, right = lax.fori_loop(0, chunks, look_up, (zero, zero))
    send_halo(0, cond_p, left, right)
    greeted(0)
    greet(1)
    for copy in loads[1:]:
        copy.wait()
    take_halo(0, cond_p)

    lane = lanes_of(tile)
    one = jnp.float32(1.0)
    beside_x = 4.0 - jnp.where((lane == 0) & (ix == 0), one, 0.0)
    beside_x = beside_x - jnp.where((lane == cols - 1) & (ix == nx - 1), one, 0.0)
    cond_left, cond_right = rcol[0, 0], rcol[0, 1]

    def precondition(k, carry):
        left, right, energy = carry
        here = cond_p[at(k, 8), :]
        near = around(
            k, cond_p[at(k), :], here, cond_p[at(k, 16), :], cond_left, cond_right
        )
        row = sub + 8 * k
        beside = beside_x - jnp.where((row == 0) & (iz == 0), one, 0.0)
        beside = beside - jnp.where((row == rows - 1) & (iz == nz - 1), one, 0.0)
        diagonal = 0.5 * (beside * here + near)
        diagonal = diagonal + via_conductance * via[at(k), :].astype(jnp.float32)
        diagonal = diagonal + (
            pad_conductance * pad[at(k), :].astype(jnp.float32) + leakage
        )
        inverse = 1.0 / diagonal
        resid = cur[at(k), :]
        value = resid * inverse
        inv[at(k), :] = inverse
        z_p[at(k, 8), :] = value
        left, right = packed(k, value, left, right)
        return left, right, energy + fold(resid * value)

    left, right, energy = lax.fori_loop(0, chunks, precondition, (zero, zero, zero))
    to_other(0, z_p, zother).start()
    send_halo(1, z_p, left, right)
    greeted(1)
    greet(2)
    save_z = pltpu.make_async_copy(z_p.at[pl.ds(8, rows)], z_hbm, out_sem.at[0])
    save_z.start()
    take_halo(1, z_p)
    to_other(0, z_p, zother).wait_recv()

    def image(k, field, lead, left, right, other):
        conds = [cond_p[at(k, 8 * i), :] for i in range(3)]
        values = [field[at(k, 8 * i), :] for i in range(3)]
        flux = [a * b for a, b in zip(conds, values)]
        plain = around(k, *values, left, right)
        scaled = around(k, *flux, cond_left * left, cond_right * right)
        across = via_conductance * via[at(k), :].astype(jnp.float32) * other[at(k), :]
        return lead - 0.5 * (conds[1] * plain + scaled) - across, values[1]

    z_left, z_right = rcol[1, 0], rcol[1, 1]

    def first_image(k, carry):
        left, right, curve = carry
        out, value = image(k, z_p, cur[at(k), :], z_left, z_right, zother)
        w[at(k), :] = out
        nxt = out * inv[at(k), :]
        y_p[at(k, 8), :] = nxt
        left, right = packed(k, nxt, left, right)
        return left, right, curve + fold(value * out)

    left, right, curve = lax.fori_loop(0, chunks, first_image, (zero, zero, zero))
    to_other(1, y_p, yother).start()
    send_halo(2, y_p, left, right)
    greeted(2)
    greet(3)
    save_w = pltpu.make_async_copy(w, w_hbm, out_sem.at[1])
    save_w.start()
    save_y = pltpu.make_async_copy(y_p.at[pl.ds(8, rows)], y_hbm, out_sem.at[2])
    save_y.start()
    energy = jnp.sum(energy, keepdims=True)
    curve = jnp.sum(curve, keepdims=True)
    guess = energy / curve
    take_halo(2, y_p)
    to_other(1, y_p, yother).wait_recv()

    y_left, y_right = rcol[2, 0], rcol[2, 1]

    def second_image(k, sums):
        along = w[at(k), :]
        out, nxt = image(k, y_p, along, y_left, y_right, yother)
        u[at(k), :] = out
        left_over = cur[at(k), :] - guess * along
        pre = left_over * inv[at(k), :]
        pre_image = along - guess * out
        terms = (
            left_over * pre,
            left_over * nxt,
            along * nxt,
            pre * pre_image,
            pre * out + nxt * pre_image,
            nxt * out,
        )
        return tuple(a + fold(b) for a, b in zip(sums, terms))

    sums = lax.fori_loop(0, chunks, second_image, (zero,) * 6)
    save_u = pltpu.make_async_copy(u, u_hbm, out_sem.at[3])
    save_u.start()

    line = (1, 128)
    entries = [(S0, energy), (S1, curve), (GUESS, guess)]
    entries += [
        (spot, jnp.sum(value, keepdims=True))
        for spot, value in zip((Q0, Q1, Q2, E0, E1, E2), sums)
    ]
    record = by_lane(line, entries)
    srec[...] = record
    plane[me] = record

    def in_plane(step):
        return pltpu.make_async_remote_copy(
            src_ref=srec,
            dst_ref=plane.at[me],
            send_sem=plane_ssem.at[step],
            recv_sem=plane_rsem.at[step],
            device_id=plane_peer(step),
            device_id_type=MESH,
        )

    for step in range(1, np_):
        in_plane(step).start()
    for step in range(1, np_):
        in_plane(step).wait_recv()

    records = plane[...].reshape(np_, 128)
    joint = pick(records, S0) / pick(records, S1)
    delta = joint - pick(records, GUESS, axis=1)
    first = by_lane(
        records.shape,
        [(Q0, -2.0 * delta), (Q1, -delta), (E0, -delta), (E1, -2.0 * delta)],
    )
    second = by_lane(records.shape, [(Q0, delta * delta), (E0, delta * delta)])
    records = (
        records
        + first * pltpu.roll(records, 127, 1)
        + second * pltpu.roll(records, 126, 1)
    )
    record = jnp.sum(records, axis=0, keepdims=True)
    record = jnp.where(lanes_of(line) == GUESS, joint, record)
    zrec[...] = record
    zbuf[iz] = record
    greeted(3)

    def along_z(i):
        away = (i + 1) // 2
        step = nz // 2 + away * (1 - 2 * lax.rem(i, 2))
        return pltpu.make_async_remote_copy(
            src_ref=zrec,
            dst_ref=zbuf.at[iz],
            send_sem=z_ssem.at[step],
            recv_sem=z_rsem.at[step],
            device_id={"row": lax.rem(iz + step, nz)},
            device_id_type=MESH,
        )

    for i in range(nz - 1):
        along_z(i).start()
    for i in range(nz - 1):
        along_z(i).wait_recv()

    records = zbuf[...].reshape(nz, 128)
    energy, curve = pick(records, S0), pick(records, S1)
    first_step = energy / curve
    delta = first_step - pick(records, GUESS, axis=1)
    weight = by_lane(records.shape, [(Q0, one), (Q1, -2.0 * delta), (Q2, delta * delta)])
    energy_next = jnp.sum(weight * records, keepdims=True)
    weight = by_lane(records.shape, [(E0, one), (E1, -delta), (E2, delta * delta)])
    curve_next = jnp.sum(weight * records, keepdims=True)
    ratio = energy_next / energy
    second_step = energy_next / (curve_next - ratio * energy_next / first_step)
    both = first_step + second_step * (1.0 + ratio)
    back = first_step * second_step
    scal_ref[...] = by_lane(scal_ref.shape, [(0, first_step), (1, both), (2, back)])

    for turn in range(3):
        end_halo(turn)
    to_other(0, z_p, zother).wait_send()
    to_other(1, y_p, yother).wait_send()
    for step in range(1, np_):
        in_plane(step).wait_send()
    for i in range(nz - 1):
        along_z(i).wait_send()
    for copy in (save_z, save_w, save_y, save_u):
        copy.wait()


def local(nz, nx, nc, current, node_class, class_conductance, pad_mask, via_mask):
    rows, cols = via_mask.shape
    field = jax.ShapeDtypeStruct((rows, cols), jnp.float32)
    full = pltpu.VMEM((rows, cols), jnp.float32)
    whole = pltpu.VMEM((rows, cols), jnp.int32)
    padded = pltpu.VMEM((rows + 16, cols), jnp.float32)
    hbm = pl.BlockSpec(memory_space=pl.ANY)
    dma = pltpu.SemaphoreType.DMA
    scratch = [full, whole, whole, whole, padded, padded, padded, full, full, full, full, full]
    scratch += [
        pltpu.VMEM((3, 2, 1, cols), jnp.float32),
        pltpu.VMEM((3, 2, 8, 128), jnp.float32),
        pltpu.VMEM((3, 2, 1, cols), jnp.float32),
        pltpu.VMEM((3, 2, 8, 128), jnp.float32),
        pltpu.VMEM((1, 128), jnp.float32),
        pltpu.VMEM((nx * nc, 1, 128), jnp.float32),
        pltpu.VMEM((1, 128), jnp.float32),
        pltpu.VMEM((nz, 1, 128), jnp.float32),
        dma((4,)),
        dma((4,)),
        dma((3, 4)),
        dma((3, 4)),
        dma((2,)),
        dma((2,)),
        dma((nx * nc,)),
        dma((nx * nc,)),
        dma((nz,)),
        dma((nz,)),
        pltpu.SemaphoreType.REGULAR((4,)),
    ]
    z, w, y, u, scal = pl.pallas_call(
        functools.partial(kernel, nz, nx, nc),
        out_shape=[field] * 4 + [jax.ShapeDtypeStruct((8, 128), jnp.float32)],
        in_specs=[hbm, hbm, pl.BlockSpec(memory_space=pltpu.SMEM), hbm, hbm],
        out_specs=[hbm] * 4 + [pl.BlockSpec(memory_space=pltpu.VMEM)],
        scratch_shapes=scratch,
        compiler_params=pltpu.CompilerParams(
            collective_id=0, has_side_effects=True, vmem_limit_bytes=32 * 1024 * 1024
        ),
    )(current[0], node_class[0], class_conductance, pad_mask[0], via_mask)
    first_step, both, back = scal[0, 0], scal[0, 1], scal[0, 2]
    drop = both * z - back * y
    resid = current[0] - both * w + back * u
    worst = jnp.maximum(first_step * z, drop)
    return (drop[None], resid[None], worst[None])


def solution(mesh):
    grid = P("layer", ("scen", "row"), "col")
    in_specs = (grid, grid, P("layer", None), grid, P(("scen", "row"), "col"))
    sizes = (mesh.shape["row"], mesh.shape["col"], mesh.shape["layer"])
    return jax.shard_map(
        functools.partial(local, *sizes),
        mesh=mesh,
        in_specs=in_specs,
        out_specs=(grid, grid, grid),
        check_vma=False,
    )
```

```python
import functools

import jax
import jax.numpy as jnp
from jax import lax
from jax.experimental import pallas as pl
from jax.experimental.pallas import tpu as pltpu
from jax.sharding import PartitionSpec as P

MESH = pl.DeviceIdType.MESH

via_conductance = 2.0
pad_conductance = 4.0
leakage = 0.05

S0, S1, Q0, Q1, Q2, E0, E1, E2, GUESS = range(9)


def lanes_of(shape):
    return lax.broadcasted_iota(jnp.int32, shape, len(shape) - 1)


def rows_of(shape):
    return lax.broadcasted_iota(jnp.int32, shape, len(shape) - 2)


def pick(record, lane, axis=None):
    kept = jnp.where(lanes_of(record.shape) == lane, record, 0.0)
    return jnp.sum(kept, axis=axis, keepdims=True)


def by_lane(shape, entries):
    lane = lanes_of(shape)
    out = jnp.zeros(shape, jnp.float32)
    for where, value in entries:
        out = jnp.where(lane == where, value, out)
    return out


def fold(value):
    parts = [value[:, i : i + 128] for i in range(0, value.shape[1], 128)]
    while len(parts) > 1:
        parts = [a + b for a, b in zip(parts[::2], parts[1::2])]
    return parts[0]


def kernel(
    nz,
    nx,
    nc,
    cur_hbm,
    cls_hbm,
    cc_ref,
    pad_hbm,
    via_hbm,
    cur,
    z_p,
    w,
    y_p,
    u,
    scal_ref,
    cls,
    pad,
    via,
    cond_p,
    edges,
    coupling,
    inv,
    zother,
    yother,
    srow,
    scol,
    rrow,
    rcol,
    srec,
    plane,
    zrec,
    zbuf,
    in_sem,
    halo_ssem,
    halo_rsem,
    other_ssem,
    other_rsem,
    plane_ssem,
    plane_rsem,
    z_ssem,
    z_rsem,
    ready,
):
    iz, ix, ic = lax.axis_index("row"), lax.axis_index("col"), lax.axis_index("layer")
    rows, cols = cur.shape
    unroll = 2
    chunks = rows // 8
    np_ = nx * nc
    me = ix * nc + ic

    loads = [
        pltpu.make_async_copy(src, dst, in_sem.at[i])
        for i, (src, dst) in enumerate(
            ((cls_hbm, cls), (cur_hbm, cur), (pad_hbm, pad), (via_hbm, via))
        )
    ]
    for copy in loads:
        copy.start()

    rrow[...] = jnp.zeros(rrow.shape, jnp.float32)
    rcol[...] = jnp.zeros(rcol.shape, jnp.float32)

    barrier = pltpu.get_barrier_semaphore()
    zup, zdown = lax.rem(iz + nz - 1, nz), lax.rem(iz + 1, nz)
    for near in (zup, zdown):
        pl.semaphore_signal(barrier, inc=1, device_id={"row": near}, device_id_type=MESH)

    def plane_peer(step):
        other = lax.rem(me + step, np_)
        return {"col": other // nc, "layer": lax.rem(other, nc)}

    for step in range(1, np_):
        pl.semaphore_signal(barrier, inc=1, device_id=plane_peer(step), device_id_type=MESH)
    pl.semaphore_wait(barrier, np_ + 1)

    levels = (nz // 2).bit_length() - 1

    def greet(level):
        if level >= levels:
            return
        far = 1 << level
        for near in (lax.rem(iz + far, nz), lax.rem(iz + nz - far, nz)):
            pl.semaphore_signal(
                ready.at[level], inc=1, device_id={"row": near}, device_id_type=MESH
            )

    def greeted(level):
        if level < levels:
            pl.semaphore_wait(ready.at[level], 2)

    greet(0)

    sides = (
        (srow, rrow, 0, 1, iz > 0, iz < nz - 1, {"row": iz - 1}),
        (srow, rrow, 1, 0, iz < nz - 1, iz > 0, {"row": iz + 1}),
        (scol, rcol, 0, 1, ix > 0, ix < nx - 1, {"col": ix - 1}),
        (scol, rcol, 1, 0, ix < nx - 1, ix > 0, {"col": ix + 1}),
    )

    def halo(turn, i):
        src, dst, mine, theirs, _, _, target = sides[i]
        return pltpu.make_async_remote_copy(
            src_ref=src.at[turn, mine],
            dst_ref=dst.at[turn, theirs],
            send_sem=halo_ssem.at[turn, i],
            recv_sem=halo_rsem.at[turn, i],
            device_id=target,
            device_id_type=MESH,
        )

    def send_halo(turn, field, left, right):
        srow[turn, 0] = field[8:9, :]
        srow[turn, 1] = field[rows + 7 : rows + 8, :]
        scol[turn, 0] = left
        scol[turn, 1] = right
        for i in range(4):
            pl.when(sides[i][4])(halo(turn, i).start)

    def take_halo(turn, field):
        for i in range(4):
            pl.when(sides[i][5])(halo(turn, i).wait_recv)
        field[0:8, :] = jnp.broadcast_to(rrow[turn, 0], (8, cols))
        field[rows + 8 : rows + 16, :] = jnp.broadcast_to(rrow[turn, 1], (8, cols))

    def end_halo(turn):
        for i in range(4):
            pl.when(sides[i][4])(halo(turn, i).wait_send)

    def to_other(turn, src, dst):
        return pltpu.make_async_remote_copy(
            src_ref=src.at[pl.ds(8, rows)],
            dst_ref=dst,
            send_sem=other_ssem.at[turn],
            recv_sem=other_rsem.at[turn],
            device_id={"layer": 1 - ic},
            device_id_type=MESH,
        )

    tile = (8, cols)
    block = (8, 128)
    zero = jnp.zeros(block, jnp.float32)
    sub = rows_of(tile)
    narrow_lane = lanes_of(block)

    def at(k, shift=0):
        return pl.ds(pl.multiple_of(8 * k + shift, 8), 8)

    def packed(k, value, left, right):
        here = narrow_lane == k
        left = jnp.where(here, pltpu.roll(value[:, :128], k, 1), left)
        right = jnp.where(here, pltpu.roll(value[:, cols - 128 :], k + 1, 1), right)
        return left, right

    def around(k, prev, here, after, left, right):
        up = pltpu.roll(jnp.where(sub == 7, prev, here), 1, 0)
        down = pltpu.roll(jnp.where(sub == 0, after, here), 7, 0)
        left = pltpu.roll(left, lax.rem(128 - k, 128), 1)
        right = pltpu.roll(right, 127 - k, 1)
        west = pltpu.roll(here, 1, 1)
        west = jnp.concatenate(
            [jnp.where(narrow_lane == 0, left, west[:, :128]), west[:, 128:]], axis=1
        )
        east = pltpu.roll(here, cols - 1, 1)
        east = jnp.concatenate(
            [
                east[:, : cols - 128],
                jnp.where(narrow_lane == 127, right, east[:, cols - 128 :]),
            ],
            axis=1,
        )
        return up, down, west, east

    loads[0].wait()

    def look_up(k, carry):
        klass = cls[at(k), :]
        level = [cc_ref[0, i] for i in range(8)]
        for bit in range(3):
            high = (klass & (1 << bit)) != 0
            level = [jnp.where(high, b, a) for a, b in zip(level[::2], level[1::2])]
        cond_p[at(k, 8), :] = level[0]
        return packed(k, level[0], *carry)

    left, right = lax.fori_loop(0, chunks, look_up, (zero, zero), unroll=unroll)
    send_halo(0, cond_p, left, right)
    greeted(0)
    greet(1)
    for copy in loads[1:]:
        copy.wait()
    take_halo(0, cond_p)

    cond_left, cond_right = rcol[0, 0], rcol[0, 1]

    def precondition(k, carry):
        left, right, energy = carry
        here = cond_p[at(k, 8), :]
        near = around(
            k, cond_p[at(k), :], here, cond_p[at(k, 16), :], cond_left, cond_right
        )
        near = [jnp.where(other > 0.0, 0.5 * (here + other), 0.0) for other in near]
        for i in range(4):
            edges[i, at(k), :] = near[i]
        across = via_conductance * via[at(k), :].astype(jnp.float32)
        coupling[at(k), :] = across
        diagonal = (near[0] + near[1]) + (near[2] + near[3])
        diagonal = diagonal + (
            across + pad_conductance * pad[at(k), :].astype(jnp.float32) + leakage
        )
        inverse = 1.0 / diagonal
        resid = cur[at(k), :]
        value = resid * inverse
        inv[at(k), :] = inverse
        z_p[at(k, 8), :] = value
        left, right = packed(k, value, left, right)
        return left, right, energy + fold(resid * value)

    left, right, energy = lax.fori_loop(0, chunks, precondition, (zero, zero, zero), unroll=unroll)
    to_other(0, z_p, zother).start()
    send_halo(1, z_p, left, right)
    greeted(1)
    greet(2)
    take_halo(1, z_p)
    to_other(0, z_p, zother).wait_recv()

    def image(k, field, lead, left, right, other):
        values = [field[at(k, 8 * i), :] for i in range(3)]
        near = around(k, *values, left, right)
        terms = [edges[i, at(k), :] * near[i] for i in range(4)]
        beside = (terms[0] + terms[1]) + (terms[2] + terms[3])
        return lead - beside - coupling[at(k), :] * other[at(k), :], values[1]

    z_left, z_right = rcol[1, 0], rcol[1, 1]

    def first_image(k, carry):
        left, right, curve = carry
        out, value = image(k, z_p, cur[at(k), :], z_left, z_right, zother)
        w[at(k), :] = out
        nxt = out * inv[at(k), :]
        y_p[at(k, 8), :] = nxt
        left, right = packed(k, nxt, left, right)
        return left, right, curve + fold(value * out)

    left, right, curve = lax.fori_loop(0, chunks, first_image, (zero, zero, zero), unroll=unroll)
    to_other(1, y_p, yother).start()
    send_halo(2, y_p, left, right)
    greeted(2)
    greet(3)
    energy = jnp.sum(energy, keepdims=True)
    curve = jnp.sum(curve, keepdims=True)
    guess = energy / curve
    take_halo(2, y_p)
    to_other(1, y_p, yother).wait_recv()

    y_left, y_right = rcol[2, 0], rcol[2, 1]

    def second_image(k, sums):
        along = w[at(k), :]
        out, nxt = image(k, y_p, along, y_left, y_right, yother)
        u[at(k), :] = out
        left_over = cur[at(k), :] - guess * along
        pre = left_over * inv[at(k), :]
        pre_image = along - guess * out
        terms = (
            left_over * pre,
            left_over * nxt,
            along * nxt,
            pre * pre_image,
            pre * out + nxt * pre_image,
            nxt * out,
        )
        return tuple(a + fold(b) for a, b in zip(sums, terms))

    sums = lax.fori_loop(0, chunks, second_image, (zero,) * 6, unroll=unroll)

    line = (1, 128)
    entries = [(S0, energy), (S1, curve), (GUESS, guess)]
    entries += [
        (spot, jnp.sum(value, keepdims=True))
        for spot, value in zip((Q0, Q1, Q2, E0, E1, E2), sums)
    ]
    record = by_lane(line, entries)
    srec[...] = record
    plane[me] = record

    def in_plane(step):
        return pltpu.make_async_remote_copy(
            src_ref=srec,
            dst_ref=plane.at[me],
            send_sem=plane_ssem.at[step],
            recv_sem=plane_rsem.at[step],
            device_id=plane_peer(step),
            device_id_type=MESH,
        )

    for step in range(1, np_):
        in_plane(step).start()
    for step in range(1, np_):
        in_plane(step).wait_recv()

    records = plane[...].reshape(np_, 128)
    joint = pick(records, S0) / pick(records, S1)
    delta = joint - pick(records, GUESS, axis=1)
    first = by_lane(
        records.shape,
        [(Q0, -2.0 * delta), (Q1, -delta), (E0, -delta), (E1, -2.0 * delta)],
    )
    second = by_lane(records.shape, [(Q0, delta * delta), (E0, delta * delta)])
    records = (
        records
        + first * pltpu.roll(records, 127, 1)
        + second * pltpu.roll(records, 126, 1)
    )
    record = jnp.sum(records, axis=0, keepdims=True)
    record = jnp.where(lanes_of(line) == GUESS, joint, record)
    zrec[...] = record
    zbuf[iz] = record
    greeted(3)

    def along_z(i):
        step = i // 2 + 1 if i % 2 == 0 else nz - 1 - i // 2
        return pltpu.make_async_remote_copy(
            src_ref=zrec,
            dst_ref=zbuf.at[iz],
            send_sem=z_ssem.at[step],
            recv_sem=z_rsem.at[step],
            device_id={"row": lax.rem(iz + step, nz)},
            device_id_type=MESH,
        )

    for i in range(nz - 1):
        along_z(i).start()
    for i in range(nz - 1):
        along_z(i).wait_recv()

    records = zbuf[...].reshape(nz, 128)
    energy, curve = pick(records, S0), pick(records, S1)
    first_step = energy / curve
    delta = first_step - pick(records, GUESS, axis=1)
    weight = by_lane(records.shape, [(Q0, 1.0), (Q1, -2.0 * delta), (Q2, delta * delta)])
    energy_next = jnp.sum(weight * records, keepdims=True)
    weight = by_lane(records.shape, [(E0, 1.0), (E1, -delta), (E2, delta * delta)])
    curve_next = jnp.sum(weight * records, keepdims=True)
    ratio = energy_next / energy
    second_step = energy_next / (curve_next - ratio * energy_next / first_step)
    both = first_step + second_step * (1.0 + ratio)
    back = first_step * second_step
    for i, value in enumerate((first_step, both, back)):
        scal_ref[i] = jnp.broadcast_to(value, block)

    for turn in range(3):
        end_halo(turn)
    to_other(0, z_p, zother).wait_send()
    to_other(1, y_p, yother).wait_send()
    for step in range(1, np_):
        in_plane(step).wait_send()
    for i in range(nz - 1):
        along_z(i).wait_send()


def finish(cur, z_p, w, y_p, u, scal, drop_hbm, resid_hbm, worst_hbm, drop, resid, worst, sem):
    rows, cols = cur.shape
    pieces = 4
    size = rows // pieces
    wide = [jnp.concatenate([scal[i]] * (cols // 128), axis=1) for i in range(3)]
    copies = []
    for piece in range(pieces):
        for k in range(size // 8):
            at = pl.ds(piece * size + 8 * k, 8)
            below = pl.ds(piece * size + 8 * k + 8, 8)
            z = z_p[below, :]
            new = wide[1] * z - wide[2] * y_p[below, :]
            drop[at, :] = new
            resid[at, :] = cur[at, :] - wide[1] * w[at, :] + wide[2] * u[at, :]
            worst[at, :] = jnp.maximum(wide[0] * z, new)
        part = pl.ds(piece * size, size)
        for i, (src, dst) in enumerate(
            ((drop, drop_hbm), (resid, resid_hbm), (worst, worst_hbm))
        ):
            copy = pltpu.make_async_copy(src.at[part], dst.at[part], sem.at[i, piece])
            copy.start()
            copies.append(copy)
    for copy in copies:
        copy.wait()


def local(nz, nx, nc, current, node_class, class_conductance, pad_mask, via_mask):
    rows, cols = via_mask.shape
    field = jax.ShapeDtypeStruct((rows, cols), jnp.float32)
    tall = jax.ShapeDtypeStruct((rows + 16, cols), jnp.float32)
    full = pltpu.VMEM((rows, cols), jnp.float32)
    whole = pltpu.VMEM((rows, cols), jnp.int32)
    padded = pltpu.VMEM((rows + 16, cols), jnp.float32)
    hbm = pl.BlockSpec(memory_space=pltpu.HBM)
    vmem = pl.BlockSpec(memory_space=pltpu.VMEM)
    dma = pltpu.SemaphoreType.DMA
    scratch = [whole, whole, whole, padded, pltpu.VMEM((4, rows, cols), jnp.float32)]
    scratch += [full] * 4
    scratch += [
        pltpu.VMEM((3, 2, 1, cols), jnp.float32),
        pltpu.VMEM((3, 2, 8, 128), jnp.float32),
        pltpu.VMEM((3, 2, 1, cols), jnp.float32),
        pltpu.VMEM((3, 2, 8, 128), jnp.float32),
        pltpu.VMEM((1, 128), jnp.float32),
        pltpu.VMEM((nx * nc, 1, 128), jnp.float32),
        pltpu.VMEM((1, 128), jnp.float32),
        pltpu.VMEM((nz, 1, 128), jnp.float32),
        dma((4,)),
        dma((3, 4)),
        dma((3, 4)),
        dma((2,)),
        dma((2,)),
        dma((nx * nc,)),
        dma((nx * nc,)),
        dma((nz,)),
        dma((nz,)),
        pltpu.SemaphoreType.REGULAR((4,)),
    ]
    limit = 32 * 1024 * 1024
    scalars = jax.ShapeDtypeStruct((3, 8, 128), jnp.float32)
    args = (current[0], node_class[0], class_conductance, pad_mask[0], via_mask)
    stay = [pltpu.with_memory_space_constraint(arg, pltpu.HBM) for arg in args]
    solved = pl.pallas_call(
        functools.partial(kernel, nz, nx, nc),
        out_shape=[field, tall, field, tall, field, scalars],
        in_specs=[hbm, hbm, pl.BlockSpec(memory_space=pltpu.SMEM), hbm, hbm],
        out_specs=[vmem] * 6,
        scratch_shapes=scratch,
        compiler_params=pltpu.CompilerParams(
            collective_id=0, has_side_effects=True, vmem_limit_bytes=limit
        ),
    )(*stay)
    outs = pl.pallas_call(
        finish,
        out_shape=[field] * 3,
        in_specs=[vmem] * 6,
        out_specs=[hbm] * 3,
        scratch_shapes=[full] * 3 + [dma((3, 4))],
        compiler_params=pltpu.CompilerParams(vmem_limit_bytes=limit),
    )(*solved)
    return tuple(out[None] for out in outs)


def solution(mesh):
    grid = P("layer", ("scen", "row"), "col")
    in_specs = (grid, grid, P("layer", None), grid, P(("scen", "row"), "col"))
    sizes = (mesh.shape["row"], mesh.shape["col"], mesh.shape["layer"])
    return jax.shard_map(
        functools.partial(local, *sizes),
        mesh=mesh,
        in_specs=in_specs,
        out_specs=(grid, grid, grid),
        check_vma=False,
    )
```

```python
import functools

import jax
import jax.numpy as jnp
from jax import lax
from jax.experimental import pallas as pl
from jax.experimental.pallas import tpu as pltpu
from jax.sharding import PartitionSpec as P

MESH = pl.DeviceIdType.MESH

via_conductance = 2.0
pad_conductance = 4.0
leakage = 0.05

REACH = 2

S0, S1, Q0, Q1, Q2, E0, E1, E2, GUESS = range(9)


def lanes_of(shape):
    return lax.broadcasted_iota(jnp.int32, shape, len(shape) - 1)


def rows_of(shape):
    return lax.broadcasted_iota(jnp.int32, shape, len(shape) - 2)


def pick(record, lane, axis=None):
    kept = jnp.where(lanes_of(record.shape) == lane, record, 0.0)
    return jnp.sum(kept, axis=axis, keepdims=True)


def by_lane(shape, entries):
    lane = lanes_of(shape)
    out = jnp.zeros(shape, jnp.float32)
    for where, value in entries:
        out = jnp.where(lane == where, value, out)
    return out


def fold(value):
    parts = [value[:, i : i + 128] for i in range(0, value.shape[1], 128)]
    while len(parts) > 1:
        parts = [a + b for a, b in zip(parts[::2], parts[1::2])]
    return parts[0]


def kernel(
    nz,
    nx,
    nc,
    cur_hbm,
    cls_hbm,
    cc_ref,
    pad_hbm,
    via_hbm,
    cur,
    z_p,
    w,
    y_p,
    u,
    scal_ref,
    cls,
    pad,
    via,
    cond_p,
    edges,
    coupling,
    base,
    inv,
    zother,
    yother,
    raw_row,
    raw_col,
    raw_corner,
    got_row,
    got_col,
    got_corner,
    y_row,
    y_col,
    goty_row,
    goty_col,
    srec,
    near,
    zrec,
    zbuf,
    in_sem,
    halo_ssem,
    halo_rsem,
    other_ssem,
    other_rsem,
    near_ssem,
    near_rsem,
    z_ssem,
    z_rsem,
    ready,
):
    iz, ix, ic = lax.axis_index("row"), lax.axis_index("col"), lax.axis_index("layer")
    rows, cols = cur.shape
    unroll = 2
    chunks = rows // 8
    reach = REACH
    me = ix * nc + ic

    loads = [
        pltpu.make_async_copy(src, dst, in_sem.at[i])
        for i, (src, dst) in enumerate(
            ((cls_hbm, cls), (cur_hbm, cur), (pad_hbm, pad), (via_hbm, via))
        )
    ]
    for copy in loads:
        copy.start()

    for buffer in (got_row, got_col, got_corner, goty_row, goty_col, zbuf):
        buffer[...] = jnp.zeros(buffer.shape, jnp.float32)

    def device(dz, dx, dc=0):
        where = {}
        for name, index, size, step in (
            ("row", iz, nz, dz),
            ("col", ix, nx, dx),
            ("layer", ic, nc, dc),
        ):
            if step % size:
                where[name] = lax.rem(index + step % size, size)
        return where

    plane = [(dx, dc) for dx in range(nx) for dc in range(nc)]
    greets = [(0, dx, dc) for dx, dc in plane[1:]]
    greets += [(dz, dx, 0) for dz in (-1, 1) for dx in (0, -1, 1)]
    barrier = pltpu.get_barrier_semaphore()
    for steps in greets:
        pl.semaphore_signal(
            barrier, inc=1, device_id=device(*steps), device_id_type=MESH
        )

    levels = (nz // 2).bit_length() - 1

    def greet(level):
        if level >= levels:
            return
        far = 1 << level
        for near in (lax.rem(iz + far, nz), lax.rem(iz + nz - far, nz)):
            pl.semaphore_signal(
                ready.at[level], inc=1, device_id={"row": near}, device_id_type=MESH
            )

    def greeted(level):
        if level < levels:
            pl.semaphore_wait(ready.at[level], 2)

    inside = {
        ("row", -1): iz > 0,
        ("row", 1): iz < nz - 1,
        ("col", -1): ix > 0,
        ("col", 1): ix < nx - 1,
    }

    def exists(dz, dx):
        flags = [inside["row", dz]] if dz else []
        flags += [inside["col", dx]] if dx else []
        return functools.reduce(jnp.logical_and, flags)

    slot = {-1: 0, 1: 1}
    raw = [(dz, 0, raw_row.at[slot[dz]], got_row, slot[-dz]) for dz in (-1, 1)]
    raw += [(0, dx, raw_col.at[slot[dx]], got_col, slot[-dx]) for dx in (-1, 1)]
    raw += [
        (
            dz,
            dx,
            raw_corner.at[2 * slot[dz] + slot[dx]],
            got_corner,
            2 * slot[-dz] + slot[-dx],
        )
        for dz in (-1, 1)
        for dx in (-1, 1)
    ]
    image_halo = [(dz, 0, y_row.at[slot[dz]], goty_row, slot[-dz]) for dz in (-1, 1)]
    image_halo += [(0, dx, y_col.at[slot[dx]], goty_col, slot[-dx]) for dx in (-1, 1)]

    def halo(turn, table, i):
        dz, dx, src, dst, there = table[i]
        return pltpu.make_async_remote_copy(
            src_ref=src,
            dst_ref=dst.at[there],
            send_sem=halo_ssem.at[turn, i],
            recv_sem=halo_rsem.at[turn, i],
            device_id=device(dz, dx),
            device_id_type=MESH,
        )

    def send_halo(turn, table):
        for i, (dz, dx, *_) in enumerate(table):
            pl.when(exists(dz, dx))(halo(turn, table, i).start)

    def take_halo(turn, table):
        for i, (dz, dx, *_) in enumerate(table):
            pl.when(exists(-dz, -dx))(halo(turn, table, i).wait_recv)

    def end_halo(turn, table):
        for i, (dz, dx, *_) in enumerate(table):
            pl.when(exists(dz, dx))(halo(turn, table, i).wait_send)

    def to_other(turn, src, dst):
        return pltpu.make_async_remote_copy(
            src_ref=src.at[pl.ds(8, rows)],
            dst_ref=dst,
            send_sem=other_ssem.at[turn],
            recv_sem=other_rsem.at[turn],
            device_id={"layer": 1 - ic},
            device_id_type=MESH,
        )

    tile = (8, cols)
    block = (8, 128)
    zero = jnp.zeros(block, jnp.float32)
    sub = rows_of(tile)
    narrow_lane = lanes_of(block)

    def at(k, shift=0):
        return pl.ds(pl.multiple_of(8 * k + shift, 8), 8)

    def packed(k, value, left, right):
        here = narrow_lane == k
        left = jnp.where(here, pltpu.roll(value[:, :128], k, 1), left)
        right = jnp.where(here, pltpu.roll(value[:, cols - 128 :], k + 1, 1), right)
        return left, right

    def around(k, prev, here, after, left, right):
        up = pltpu.roll(jnp.where(sub == 7, prev, here), 1, 0)
        down = pltpu.roll(jnp.where(sub == 0, after, here), 7, 0)
        left = pltpu.roll(left, lax.rem(128 - k, 128), 1)
        right = pltpu.roll(right, 127 - k, 1)
        west = pltpu.roll(here, 1, 1)
        west = jnp.concatenate(
            [jnp.where(narrow_lane == 0, left, west[:, :128]), west[:, 128:]], axis=1
        )
        east = pltpu.roll(here, cols - 1, 1)
        east = jnp.concatenate(
            [
                east[:, : cols - 128],
                jnp.where(narrow_lane == 127, right, east[:, cols - 128 :]),
            ],
            axis=1,
        )
        return up, down, west, east

    for copy in loads:
        copy.wait()
    last = cols - 128

    def place(k, value, lane, out):
        moved = pltpu.roll(value, lax.rem(k + 128 - lane, 128), 1)
        return jnp.where(narrow_lane == k, moved, out)

    def look_up(k, carry):
        klass = cls[at(k), :]
        level = [cc_ref[0, i] for i in range(8)]
        for bit in range(3):
            high = (klass & (1 << bit)) != 0
            level = [jnp.where(high, b, a) for a, b in zip(level[::2], level[1::2])]
        cond = level[0]
        cond_p[at(k, 8), :] = cond
        across = via_conductance * via[at(k), :].astype(jnp.float32)
        coupling[at(k), :] = across
        rest = across + (pad_conductance * pad[at(k), :].astype(jnp.float32) + leakage)
        base[at(k), :] = rest
        load = cur[at(k), :]
        borders = (
            (cond[:, :128], 0),
            (cond[:, :128], 1),
            (rest[:, :128], 0),
            (load[:, :128], 0),
            (cond[:, last:], 127),
            (cond[:, last:], 126),
            (rest[:, last:], 127),
            (load[:, last:], 127),
        )
        return tuple(place(k, *border, out) for border, out in zip(borders, carry))

    packs = lax.fori_loop(0, chunks, look_up, (zero,) * 8, unroll=unroll)
    for i in range(8):
        raw_col[i // 4, i % 4] = packs[i]
    for side, row in ((0, 0), (1, rows - 1)):
        inward = 1 - 2 * side
        raw_row[side, 0] = cond_p[8 + row : 9 + row, :]
        raw_row[side, 1] = cond_p[8 + row + inward : 9 + row + inward, :]
        raw_row[side, 2] = base[row : row + 1, :]
        raw_row[side, 3] = cur[row : row + 1, :]
        for end, col in ((0, 0), (1, cols - 1)):
            corner = cond_p[8 + row : 9 + row, col : col + 1]
            raw_corner[2 * side + end] = jnp.broadcast_to(corner, block)

    pl.semaphore_wait(barrier, len(greets))
    greet(0)
    send_halo(0, raw)
    greeted(0)
    greet(1)
    take_halo(0, raw)
    for side, row in ((0, 0), (1, rows + 8)):
        cond_p[row : row + 8, :] = jnp.broadcast_to(got_row[side, 0], tile)

    cond_left, cond_right = got_col[0, 0], got_col[1, 0]

    def edge(here, other):
        return jnp.where(other > 0.0, 0.5 * (here + other), 0.0)

    def precondition(k, energy):
        here = cond_p[at(k, 8), :]
        sides = around(
            k, cond_p[at(k), :], here, cond_p[at(k, 16), :], cond_left, cond_right
        )
        sides = [edge(here, other) for other in sides]
        for i in range(4):
            edges[i, at(k), :] = sides[i]
        diagonal = ((sides[0] + sides[1]) + (sides[2] + sides[3])) + base[at(k), :]
        inverse = 1.0 / diagonal
        resid = cur[at(k), :]
        value = resid * inverse
        inv[at(k), :] = inverse
        z_p[at(k, 8), :] = value
        return energy + fold(resid * value)

    energy = lax.fori_loop(0, chunks, precondition, zero, unroll=unroll)
    to_other(0, z_p, zother).start()
    greeted(1)
    greet(2)

    def beyond(here, others, rest, load):
        sides = [edge(here, other) for other in others]
        diagonal = ((sides[0] + sides[1]) + (sides[2] + sides[3])) + rest
        return jnp.where(here > 0.0, load * (1.0 / diagonal), 0.0)

    for side, row, inner in ((0, 0, 8), (1, rows + 8, rows + 7)):
        here, outer, rest, load = [
            jnp.broadcast_to(got_row[side, i], tile) for i in range(4)
        ]
        inner = jnp.broadcast_to(cond_p[inner : inner + 1, :], tile)
        west = pltpu.roll(here, 1, 1)
        west = jnp.concatenate(
            [
                jnp.where(narrow_lane == 0, got_corner[2 * side], west[:, :128]),
                west[:, 128:],
            ],
            axis=1,
        )
        east = pltpu.roll(here, cols - 1, 1)
        east = jnp.concatenate(
            [
                east[:, :last],
                jnp.where(narrow_lane == 127, got_corner[2 * side + 1], east[:, last:]),
            ],
            axis=1,
        )
        z_p[row : row + 8, :] = beyond(here, (outer, inner, west, east), rest, load)

    narrow_sub = rows_of(block)
    z_ends = []
    for side in range(2):
        here, outer, rest, load = [got_col[side, i] for i in range(4)]
        up = pltpu.roll(here, 1, 0)
        up = jnp.where(narrow_sub == 0, pltpu.roll(up, 1, 1), up)
        up = jnp.where((narrow_sub == 0) & (narrow_lane == 0), got_corner[side], up)
        down = pltpu.roll(here, 7, 0)
        down = jnp.where(narrow_sub == 7, pltpu.roll(down, 127, 1), down)
        end = (narrow_sub == 7) & (narrow_lane == chunks - 1)
        down = jnp.where(end, got_corner[2 + side], down)
        inner = raw_col[side, 0]
        z_ends.append(beyond(here, (up, down, outer, inner), rest, load))
    z_left, z_right = z_ends
    to_other(0, z_p, zother).wait_recv()

    def image(k, field, lead, left, right, other):
        values = [field[at(k, 8 * i), :] for i in range(3)]
        sides = around(k, *values, left, right)
        terms = [edges[i, at(k), :] * sides[i] for i in range(4)]
        beside = (terms[0] + terms[1]) + (terms[2] + terms[3])
        return lead - beside - coupling[at(k), :] * other[at(k), :], values[1]

    def first_image(k, carry):
        left, right, curve = carry
        out, value = image(k, z_p, cur[at(k), :], z_left, z_right, zother)
        w[at(k), :] = out
        nxt = out * inv[at(k), :]
        y_p[at(k, 8), :] = nxt
        left, right = packed(k, nxt, left, right)
        return left, right, curve + fold(value * out)

    left, right, curve = lax.fori_loop(0, chunks, first_image, (zero, zero, zero), unroll=unroll)
    to_other(1, y_p, yother).start()
    y_row[0] = y_p[8:9, :]
    y_row[1] = y_p[rows + 7 : rows + 8, :]
    y_col[0] = left
    y_col[1] = right
    send_halo(1, image_halo)
    greeted(2)
    greet(3)
    energy = jnp.sum(energy, keepdims=True)
    curve = jnp.sum(curve, keepdims=True)
    guess = energy / curve
    take_halo(1, image_halo)
    for side, row in ((0, 0), (1, rows + 8)):
        y_p[row : row + 8, :] = jnp.broadcast_to(goty_row[side], tile)
    to_other(1, y_p, yother).wait_recv()

    y_left, y_right = goty_col[0], goty_col[1]

    def second_image(k, sums):
        along = w[at(k), :]
        out, nxt = image(k, y_p, along, y_left, y_right, yother)
        u[at(k), :] = out
        left_over = cur[at(k), :] - guess * along
        pre = left_over * inv[at(k), :]
        pre_image = along - guess * out
        terms = (
            left_over * pre,
            left_over * nxt,
            along * nxt,
            pre * pre_image,
            pre * out + nxt * pre_image,
            nxt * out,
        )
        return tuple(a + fold(b) for a, b in zip(sums, terms))

    sums = lax.fori_loop(0, chunks, second_image, (zero,) * 6, unroll=unroll)

    line = (1, 128)
    entries = [(S0, energy), (S1, curve), (GUESS, guess)]
    entries += [
        (spot, jnp.sum(value, keepdims=True))
        for spot, value in zip((Q0, Q1, Q2, E0, E1, E2), sums)
    ]
    record = by_lane(line, entries)
    srec[...] = record
    near[reach, me] = record

    shifts = [0] + [dz for far in range(1, reach + 1) for dz in (far, -far)]
    hops = [(dz, i) for dz in shifts for i in range(len(plane)) if dz or i]

    def close(dz, i):
        return pltpu.make_async_remote_copy(
            src_ref=srec,
            dst_ref=near.at[reach - dz, me],
            send_sem=near_ssem.at[reach - dz, i],
            recv_sem=near_rsem.at[reach - dz, i],
            device_id=device(dz, *plane[i]),
            device_id_type=MESH,
        )

    for hop in hops:
        close(*hop).start()
    for hop in hops:
        if not hop[0]:
            close(*hop).wait_recv()

    records = near[reach].reshape(len(plane), 128)
    joint = pick(records, S0) / pick(records, S1)
    delta = joint - pick(records, GUESS, axis=1)
    first = by_lane(
        records.shape,
        [(Q0, -2.0 * delta), (Q1, -delta), (E0, -delta), (E1, -2.0 * delta)],
    )
    second = by_lane(records.shape, [(Q0, delta * delta), (E0, delta * delta)])
    records = (
        records
        + first * pltpu.roll(records, 127, 1)
        + second * pltpu.roll(records, 126, 1)
    )
    record = jnp.sum(records, axis=0, keepdims=True)
    record = jnp.where(lanes_of(line) == GUESS, joint, record)
    zrec[...] = record
    greeted(3)

    far = [i for pair in zip(range(1, nz), range(nz - 1, 0, -1)) for i in pair]
    far = [i for i in dict.fromkeys(far) if reach < i < nz - reach]

    def along_z(step):
        return pltpu.make_async_remote_copy(
            src_ref=zrec,
            dst_ref=zbuf.at[iz],
            send_sem=z_ssem.at[step],
            recv_sem=z_rsem.at[step],
            device_id=device(step, 0),
            device_id_type=MESH,
        )

    for step in far:
        along_z(step).start()
    for step in far:
        along_z(step).wait_recv()
    for hop in hops:
        if hop[0]:
            close(*hop).wait_recv()

    records = [near[i].reshape(len(plane), 128) for i in range(2 * reach + 1)]
    records = jnp.concatenate(records + [zbuf[...].reshape(nz, 128)], axis=0)
    energy, curve = pick(records, S0), pick(records, S1)
    first_step = energy / curve
    delta = first_step - pick(records, GUESS, axis=1)
    weight = by_lane(records.shape, [(Q0, 1.0), (Q1, -2.0 * delta), (Q2, delta * delta)])
    energy_next = jnp.sum(weight * records, keepdims=True)
    weight = by_lane(records.shape, [(E0, 1.0), (E1, -delta), (E2, delta * delta)])
    curve_next = jnp.sum(weight * records, keepdims=True)
    ratio = energy_next / energy
    second_step = energy_next / (curve_next - ratio * energy_next / first_step)
    both = first_step + second_step * (1.0 + ratio)
    back = first_step * second_step
    for i, value in enumerate((first_step, both, back)):
        scal_ref[i] = jnp.broadcast_to(value, block)

    end_halo(0, raw)
    end_halo(1, image_halo)
    to_other(0, z_p, zother).wait_send()
    to_other(1, y_p, yother).wait_send()
    for hop in hops:
        close(*hop).wait_send()
    for step in far:
        along_z(step).wait_send()


def finish(cur, z_p, w, y_p, u, scal, drop_hbm, resid_hbm, worst_hbm, drop, resid, worst, sem):
    rows, cols = cur.shape
    pieces = 4
    size = rows // pieces
    wide = [jnp.concatenate([scal[i]] * (cols // 128), axis=1) for i in range(3)]
    copies = []
    for piece in range(pieces):
        for k in range(size // 8):
            at = pl.ds(piece * size + 8 * k, 8)
            below = pl.ds(piece * size + 8 * k + 8, 8)
            z = z_p[below, :]
            new = wide[1] * z - wide[2] * y_p[below, :]
            drop[at, :] = new
            resid[at, :] = cur[at, :] - wide[1] * w[at, :] + wide[2] * u[at, :]
            worst[at, :] = jnp.maximum(wide[0] * z, new)
        part = pl.ds(piece * size, size)
        for i, (src, dst) in enumerate(
            ((drop, drop_hbm), (resid, resid_hbm), (worst, worst_hbm))
        ):
            copy = pltpu.make_async_copy(src.at[part], dst.at[part], sem.at[i, piece])
            copy.start()
            copies.append(copy)
    for copy in copies:
        copy.wait()


def local(nz, nx, nc, current, node_class, class_conductance, pad_mask, via_mask):
    rows, cols = via_mask.shape
    field = jax.ShapeDtypeStruct((rows, cols), jnp.float32)
    tall = jax.ShapeDtypeStruct((rows + 16, cols), jnp.float32)
    full = pltpu.VMEM((rows, cols), jnp.float32)
    whole = pltpu.VMEM((rows, cols), jnp.int32)
    padded = pltpu.VMEM((rows + 16, cols), jnp.float32)
    hbm = pl.BlockSpec(memory_space=pltpu.HBM)
    vmem = pl.BlockSpec(memory_space=pltpu.VMEM)
    dma = pltpu.SemaphoreType.DMA
    scratch = [whole, whole, whole, padded, pltpu.VMEM((4, rows, cols), jnp.float32)]
    scratch += [full] * 5
    near = (2 * REACH + 1, nx * nc)
    scratch += [
        pltpu.VMEM((2, 4, 1, cols), jnp.float32),
        pltpu.VMEM((2, 4, 8, 128), jnp.float32),
        pltpu.VMEM((4, 8, 128), jnp.float32),
    ] * 2
    scratch += [
        pltpu.VMEM((2, 1, cols), jnp.float32),
        pltpu.VMEM((2, 8, 128), jnp.float32),
    ] * 2
    scratch += [
        pltpu.VMEM((1, 128), jnp.float32),
        pltpu.VMEM((*near, 1, 128), jnp.float32),
        pltpu.VMEM((1, 128), jnp.float32),
        pltpu.VMEM((nz, 1, 128), jnp.float32),
        dma((4,)),
        dma((2, 8)),
        dma((2, 8)),
        dma((2,)),
        dma((2,)),
        dma(near),
        dma(near),
        dma((nz,)),
        dma((nz,)),
        pltpu.SemaphoreType.REGULAR((4,)),
    ]
    limit = 32 * 1024 * 1024
    scalars = jax.ShapeDtypeStruct((3, 8, 128), jnp.float32)
    args = (current[0], node_class[0], class_conductance, pad_mask[0], via_mask)
    stay = [pltpu.with_memory_space_constraint(arg, pltpu.HBM) for arg in args]
    solved = pl.pallas_call(
        functools.partial(kernel, nz, nx, nc),
        out_shape=[field, tall, field, tall, field, scalars],
        in_specs=[hbm, hbm, pl.BlockSpec(memory_space=pltpu.SMEM), hbm, hbm],
        out_specs=[vmem] * 6,
        scratch_shapes=scratch,
        compiler_params=pltpu.CompilerParams(
            collective_id=0, has_side_effects=True, vmem_limit_bytes=limit
        ),
    )(*stay)
    outs = pl.pallas_call(
        finish,
        out_shape=[field] * 3,
        in_specs=[vmem] * 6,
        out_specs=[hbm] * 3,
        scratch_shapes=[full] * 3 + [dma((3, 4))],
        compiler_params=pltpu.CompilerParams(vmem_limit_bytes=limit),
    )(*solved)
    return tuple(out[None] for out in outs)


def solution(mesh):
    grid = P("layer", ("scen", "row"), "col")
    in_specs = (grid, grid, P("layer", None), grid, P(("scen", "row"), "col"))
    sizes = (mesh.shape["row"], mesh.shape["col"], mesh.shape["layer"])
    return jax.shard_map(
        functools.partial(local, *sizes),
        mesh=mesh,
        in_specs=in_specs,
        out_specs=(grid, grid, grid),
        check_vma=False,
    )
```

```python
import functools

import jax
import jax.numpy as jnp
from jax import lax
from jax.experimental import pallas as pl
from jax.experimental.pallas import tpu as pltpu
from jax.sharding import PartitionSpec as P

MESH = pl.DeviceIdType.MESH

via_conductance = 2.0
pad_conductance = 4.0
leakage = 0.05

REACH = 2

S0, S1, Q0, Q1, Q2, E0, E1, E2, GUESS = range(9)


def lanes_of(shape):
    return lax.broadcasted_iota(jnp.int32, shape, len(shape) - 1)


def rows_of(shape):
    return lax.broadcasted_iota(jnp.int32, shape, len(shape) - 2)


def pick(record, lane, axis=None):
    kept = jnp.where(lanes_of(record.shape) == lane, record, 0.0)
    return jnp.sum(kept, axis=axis, keepdims=True)


def by_lane(shape, entries):
    lane = lanes_of(shape)
    out = jnp.zeros(shape, jnp.float32)
    for where, value in entries:
        out = jnp.where(lane == where, value, out)
    return out


def fold(value):
    parts = [value[:, i : i + 128] for i in range(0, value.shape[1], 128)]
    while len(parts) > 1:
        parts = [a + b for a, b in zip(parts[::2], parts[1::2])]
    return parts[0]


def kernel(
    nz,
    nx,
    nc,
    cur_hbm,
    cls_hbm,
    cc_ref,
    pad_hbm,
    via_hbm,
    cur,
    z_p,
    w,
    y_p,
    u,
    scal_ref,
    cls,
    pad,
    via,
    cond_p,
    edges,
    coupling,
    base,
    inv,
    zother,
    yother,
    raw_row,
    raw_col,
    raw_corner,
    got_row,
    got_col,
    got_corner,
    y_row,
    y_col,
    goty_row,
    goty_col,
    srec,
    near,
    zrec,
    zbuf,
    in_sem,
    halo_ssem,
    halo_rsem,
    other_ssem,
    other_rsem,
    near_ssem,
    near_rsem,
    z_ssem,
    z_rsem,
    low,
    zero_in,
    high,
):
    iz, ix, ic = lax.axis_index("row"), lax.axis_index("col"), lax.axis_index("layer")
    rows, cols = cur.shape
    unroll = 2
    chunks = rows // 8
    reach = REACH
    me = ix * nc + ic

    loads = [
        pltpu.make_async_copy(src, dst, in_sem.at[i])
        for i, (src, dst) in enumerate(
            ((cls_hbm, cls), (cur_hbm, cur), (pad_hbm, pad), (via_hbm, via))
        )
    ]
    for copy in loads:
        copy.start()

    for buffer in (got_row, got_col, got_corner, goty_row, goty_col, zbuf):
        buffer[...] = jnp.zeros(buffer.shape, jnp.float32)

    def device(dz, dx, dc=0):
        where = {}
        for name, index, size, step in (
            ("row", iz, nz, dz),
            ("col", ix, nx, dx),
            ("layer", ic, nc, dc),
        ):
            if step % size:
                where[name] = lax.rem(index + step % size, size)
        return where

    plane = [(dx, dc) for dx in range(nx) for dc in range(nc)]
    greets = {0: [(0, dx, dc) for dx, dc in plane[1:]]}
    greets |= {dz: [(dz, dx, 0) for dx in (0, -1, 1)] for dz in (-1, 1)}
    beside = {0: True, -1: iz > 0, 1: iz < nz - 1}
    barrier = pltpu.get_barrier_semaphore()

    def greet(dz):
        for steps in greets[dz]:
            pl.semaphore_signal(
                barrier, inc=1, device_id=device(*steps), device_id_type=MESH
            )

    for dz in greets:
        pl.when(beside[dz])(functools.partial(greet, dz))

    early = nz - 5

    def tell(semaphore, row):
        pl.semaphore_signal(
            semaphore, inc=1, device_id={"row": row}, device_id_type=MESH
        )

    def announce():
        pl.when(iz >= 2)(lambda: pl.semaphore_wait(low, 1))
        pl.when((iz >= 1) & (iz < nz - 1))(lambda: tell(low, iz + 1))

        def one(row, carry):
            tell(high.at[iz], row)
            return carry

        lax.fori_loop(1, iz, one, 0)

    def learn(row):
        pl.semaphore_wait(high.at[row], 1)
        pl.when(iz == 1)(lambda: tell(high.at[row], 0))
        pl.when(iz == 0)(lambda: tell(zero_in, row))

    def meet(row):
        known = (iz <= 1) & (row <= jnp.maximum(early, 1))
        pl.when((row > iz) & jnp.logical_not(known))(lambda: learn(row))
        pl.when((row == 0) & (iz >= 2))(lambda: pl.semaphore_wait(zero_in, 1))

    def learn_early():
        def one(row, carry):
            learn(row)
            return carry

        lax.fori_loop(2, early + 1, one, 0)

    inside = {
        ("row", -1): iz > 0,
        ("row", 1): iz < nz - 1,
        ("col", -1): ix > 0,
        ("col", 1): ix < nx - 1,
    }

    def exists(dz, dx):
        flags = [inside["row", dz]] if dz else []
        flags += [inside["col", dx]] if dx else []
        return functools.reduce(jnp.logical_and, flags)

    slot = {-1: 0, 1: 1}
    raw = [(dz, 0, raw_row.at[slot[dz]], got_row, slot[-dz]) for dz in (-1, 1)]
    raw += [(0, dx, raw_col.at[slot[dx]], got_col, slot[-dx]) for dx in (-1, 1)]
    raw += [
        (
            dz,
            dx,
            raw_corner.at[2 * slot[dz] + slot[dx]],
            got_corner,
            2 * slot[-dz] + slot[-dx],
        )
        for dz in (-1, 1)
        for dx in (-1, 1)
    ]
    image_halo = [(dz, 0, y_row.at[slot[dz]], goty_row, slot[-dz]) for dz in (-1, 1)]
    image_halo += [(0, dx, y_col.at[slot[dx]], goty_col, slot[-dx]) for dx in (-1, 1)]

    def halo(turn, table, i):
        dz, dx, src, dst, there = table[i]
        return pltpu.make_async_remote_copy(
            src_ref=src,
            dst_ref=dst.at[there],
            send_sem=halo_ssem.at[turn, i],
            recv_sem=halo_rsem.at[turn, i],
            device_id=device(dz, dx),
            device_id_type=MESH,
        )

    def send_halo(turn, table):
        for i, (dz, dx, *_) in enumerate(table):
            pl.when(exists(dz, dx))(halo(turn, table, i).start)

    def take_halo(turn, table):
        for i, (dz, dx, *_) in enumerate(table):
            pl.when(exists(-dz, -dx))(halo(turn, table, i).wait_recv)

    def end_halo(turn, table):
        for i, (dz, dx, *_) in enumerate(table):
            pl.when(exists(dz, dx))(halo(turn, table, i).wait_send)

    def to_other(turn, src, dst):
        return pltpu.make_async_remote_copy(
            src_ref=src.at[pl.ds(8, rows)],
            dst_ref=dst,
            send_sem=other_ssem.at[turn],
            recv_sem=other_rsem.at[turn],
            device_id={"layer": 1 - ic},
            device_id_type=MESH,
        )

    tile = (8, cols)
    block = (8, 128)
    zero = jnp.zeros(block, jnp.float32)
    sub = rows_of(tile)
    narrow_lane = lanes_of(block)

    def at(k, shift=0):
        return pl.ds(pl.multiple_of(8 * k + shift, 8), 8)

    def packed(k, value, left, right):
        here = narrow_lane == k
        left = jnp.where(here, pltpu.roll(value[:, :128], k, 1), left)
        right = jnp.where(here, pltpu.roll(value[:, cols - 128 :], k + 1, 1), right)
        return left, right

    def around(k, prev, here, after, left, right):
        up = pltpu.roll(jnp.where(sub == 7, prev, here), 1, 0)
        down = pltpu.roll(jnp.where(sub == 0, after, here), 7, 0)
        left = pltpu.roll(left, lax.rem(128 - k, 128), 1)
        right = pltpu.roll(right, 127 - k, 1)
        west = pltpu.roll(here, 1, 1)
        west = jnp.concatenate(
            [jnp.where(narrow_lane == 0, left, west[:, :128]), west[:, 128:]], axis=1
        )
        east = pltpu.roll(here, cols - 1, 1)
        east = jnp.concatenate(
            [
                east[:, : cols - 128],
                jnp.where(narrow_lane == 127, right, east[:, cols - 128 :]),
            ],
            axis=1,
        )
        return up, down, west, east

    for copy in loads:
        copy.wait()
    last = cols - 128

    def place(k, value, lane, out):
        moved = pltpu.roll(value, lax.rem(k + 128 - lane, 128), 1)
        return jnp.where(narrow_lane == k, moved, out)

    def look_up(k, carry):
        klass = cls[at(k), :]
        level = [cc_ref[0, i] for i in range(8)]
        for bit in range(3):
            high = (klass & (1 << bit)) != 0
            level = [jnp.where(high, b, a) for a, b in zip(level[::2], level[1::2])]
        cond = level[0]
        cond_p[at(k, 8), :] = cond
        across = via_conductance * via[at(k), :].astype(jnp.float32)
        coupling[at(k), :] = across
        rest = across + (pad_conductance * pad[at(k), :].astype(jnp.float32) + leakage)
        base[at(k), :] = rest
        load = cur[at(k), :]
        borders = (
            (cond[:, :128], 0),
            (cond[:, :128], 1),
            (rest[:, :128], 0),
            (load[:, :128], 0),
            (cond[:, last:], 127),
            (cond[:, last:], 126),
            (rest[:, last:], 127),
            (load[:, last:], 127),
        )
        return tuple(place(k, *border, out) for border, out in zip(borders, carry))

    packs = lax.fori_loop(0, chunks, look_up, (zero,) * 8, unroll=unroll)
    for i in range(8):
        raw_col[i // 4, i % 4] = packs[i]
    for side, row in ((0, 0), (1, rows - 1)):
        inward = 1 - 2 * side
        raw_row[side, 0] = cond_p[8 + row : 9 + row, :]
        raw_row[side, 1] = cond_p[8 + row + inward : 9 + row + inward, :]
        raw_row[side, 2] = base[row : row + 1, :]
        raw_row[side, 3] = cur[row : row + 1, :]
        for end, col in ((0, 0), (1, cols - 1)):
            corner = cond_p[8 + row : 9 + row, col : col + 1]
            raw_corner[2 * side + end] = jnp.broadcast_to(corner, block)

    neighbours = jnp.minimum(iz, 1) + jnp.minimum(nz - 1 - iz, 1)
    pl.semaphore_wait(barrier, len(greets[0]) + len(greets[1]) * neighbours)
    send_halo(0, raw)
    announce()
    pl.when(iz <= 1)(learn_early)
    take_halo(0, raw)
    for side, row in ((0, 0), (1, rows + 8)):
        cond_p[row : row + 8, :] = jnp.broadcast_to(got_row[side, 0], tile)

    cond_left, cond_right = got_col[0, 0], got_col[1, 0]

    def edge(here, other):
        return jnp.where(other > 0.0, 0.5 * (here + other), 0.0)

    def precondition(k, energy):
        here = cond_p[at(k, 8), :]
        sides = around(
            k, cond_p[at(k), :], here, cond_p[at(k, 16), :], cond_left, cond_right
        )
        sides = [edge(here, other) for other in sides]
        for i in range(4):
            edges[i, at(k), :] = sides[i]
        diagonal = ((sides[0] + sides[1]) + (sides[2] + sides[3])) + base[at(k), :]
        inverse = 1.0 / diagonal
        resid = cur[at(k), :]
        value = resid * inverse
        inv[at(k), :] = inverse
        z_p[at(k, 8), :] = value
        return energy + fold(resid * value)

    energy = lax.fori_loop(0, chunks, precondition, zero, unroll=unroll)
    to_other(0, z_p, zother).start()

    def beyond(here, others, rest, load):
        sides = [edge(here, other) for other in others]
        diagonal = ((sides[0] + sides[1]) + (sides[2] + sides[3])) + rest
        return jnp.where(here > 0.0, load * (1.0 / diagonal), 0.0)

    for side, row, inner in ((0, 0, 8), (1, rows + 8, rows + 7)):
        here, outer, rest, load = [
            jnp.broadcast_to(got_row[side, i], tile) for i in range(4)
        ]
        inner = jnp.broadcast_to(cond_p[inner : inner + 1, :], tile)
        west = pltpu.roll(here, 1, 1)
        west = jnp.concatenate(
            [
                jnp.where(narrow_lane == 0, got_corner[2 * side], west[:, :128]),
                west[:, 128:],
            ],
            axis=1,
        )
        east = pltpu.roll(here, cols - 1, 1)
        east = jnp.concatenate(
            [
                east[:, :last],
                jnp.where(narrow_lane == 127, got_corner[2 * side + 1], east[:, last:]),
            ],
            axis=1,
        )
        z_p[row : row + 8, :] = beyond(here, (outer, inner, west, east), rest, load)

    narrow_sub = rows_of(block)
    z_ends = []
    for side in range(2):
        here, outer, rest, load = [got_col[side, i] for i in range(4)]
        up = pltpu.roll(here, 1, 0)
        up = jnp.where(narrow_sub == 0, pltpu.roll(up, 1, 1), up)
        up = jnp.where((narrow_sub == 0) & (narrow_lane == 0), got_corner[side], up)
        down = pltpu.roll(here, 7, 0)
        down = jnp.where(narrow_sub == 7, pltpu.roll(down, 127, 1), down)
        end = (narrow_sub == 7) & (narrow_lane == chunks - 1)
        down = jnp.where(end, got_corner[2 + side], down)
        inner = raw_col[side, 0]
        z_ends.append(beyond(here, (up, down, outer, inner), rest, load))
    z_left, z_right = z_ends
    to_other(0, z_p, zother).wait_recv()

    def image(k, field, lead, left, right, other):
        values = [field[at(k, 8 * i), :] for i in range(3)]
        sides = around(k, *values, left, right)
        terms = [edges[i, at(k), :] * sides[i] for i in range(4)]
        beside = (terms[0] + terms[1]) + (terms[2] + terms[3])
        return lead - beside - coupling[at(k), :] * other[at(k), :], values[1]

    def first_image(k, carry):
        left, right, curve = carry
        out, value = image(k, z_p, cur[at(k), :], z_left, z_right, zother)
        w[at(k), :] = out
        nxt = out * inv[at(k), :]
        y_p[at(k, 8), :] = nxt
        left, right = packed(k, nxt, left, right)
        return left, right, curve + fold(value * out)

    left, right, curve = lax.fori_loop(0, chunks, first_image, (zero, zero, zero), unroll=unroll)
    to_other(1, y_p, yother).start()
    y_row[0] = y_p[8:9, :]
    y_row[1] = y_p[rows + 7 : rows + 8, :]
    y_col[0] = left
    y_col[1] = right
    send_halo(1, image_halo)
    energy = jnp.sum(energy, keepdims=True)
    curve = jnp.sum(curve, keepdims=True)
    guess = energy / curve
    take_halo(1, image_halo)
    for side, row in ((0, 0), (1, rows + 8)):
        y_p[row : row + 8, :] = jnp.broadcast_to(goty_row[side], tile)
    to_other(1, y_p, yother).wait_recv()

    y_left, y_right = goty_col[0], goty_col[1]

    def second_image(k, sums):
        along = w[at(k), :]
        out, nxt = image(k, y_p, along, y_left, y_right, yother)
        u[at(k), :] = out
        left_over = cur[at(k), :] - guess * along
        pre = left_over * inv[at(k), :]
        pre_image = along - guess * out
        terms = (
            left_over * pre,
            left_over * nxt,
            along * nxt,
            pre * pre_image,
            pre * out + nxt * pre_image,
            nxt * out,
        )
        return tuple(a + fold(b) for a, b in zip(sums, terms))

    sums = lax.fori_loop(0, chunks, second_image, (zero,) * 6, unroll=unroll)

    line = (1, 128)
    entries = [(S0, energy), (S1, curve), (GUESS, guess)]
    entries += [
        (spot, jnp.sum(value, keepdims=True))
        for spot, value in zip((Q0, Q1, Q2, E0, E1, E2), sums)
    ]
    record = by_lane(line, entries)
    srec[...] = record
    near[reach, me] = record

    shifts = [0] + [dz for far in range(1, reach + 1) for dz in (far, -far)]
    hops = [(dz, i) for dz in shifts for i in range(len(plane)) if dz or i]

    def close(dz, i):
        return pltpu.make_async_remote_copy(
            src_ref=srec,
            dst_ref=near.at[reach - dz, me],
            send_sem=near_ssem.at[reach - dz, i],
            recv_sem=near_rsem.at[reach - dz, i],
            device_id=device(dz, *plane[i]),
            device_id_type=MESH,
        )

    for dz in shifts:
        if dz:
            meet(lax.rem(iz + dz + nz, nz))
        for hop in hops:
            if hop[0] == dz:
                close(*hop).start()
    for hop in hops:
        if not hop[0]:
            close(*hop).wait_recv()

    records = near[reach].reshape(len(plane), 128)
    joint = pick(records, S0) / pick(records, S1)
    delta = joint - pick(records, GUESS, axis=1)
    first = by_lane(
        records.shape,
        [(Q0, -2.0 * delta), (Q1, -delta), (E0, -delta), (E1, -2.0 * delta)],
    )
    second = by_lane(records.shape, [(Q0, delta * delta), (E0, delta * delta)])
    records = (
        records
        + first * pltpu.roll(records, 127, 1)
        + second * pltpu.roll(records, 126, 1)
    )
    record = jnp.sum(records, axis=0, keepdims=True)
    record = jnp.where(lanes_of(line) == GUESS, joint, record)
    zrec[...] = record

    def along_z(row):
        return pltpu.make_async_remote_copy(
            src_ref=zrec,
            dst_ref=zbuf.at[iz],
            send_sem=z_ssem.at[row],
            recv_sem=z_rsem.at[iz],
            device_id={"row": row},
            device_id_type=MESH,
        )

    def from_z(row):
        return pltpu.make_async_remote_copy(
            src_ref=zrec,
            dst_ref=zbuf.at[row],
            send_sem=z_ssem.at[row],
            recv_sem=z_rsem.at[row],
            device_id={"row": row},
            device_id_type=MESH,
        )

    def far_rows(first, stop, act):
        def one(row, carry):
            away = jnp.abs(row - iz)
            pl.when((away > reach) & (away < nz - reach))(lambda: act(row))
            return carry

        lax.fori_loop(first, stop, one, 0)

    def met_send(row):
        meet(row)
        along_z(row).start()

    far_rows(1, iz, lambda row: along_z(row).start())
    far_rows(0, jnp.minimum(iz, 1), met_send)
    far_rows(iz + 1, nz, met_send)
    far_rows(0, nz, lambda row: from_z(row).wait_recv())
    for hop in hops:
        if hop[0]:
            close(*hop).wait_recv()

    records = [near[i].reshape(len(plane), 128) for i in range(2 * reach + 1)]
    records = jnp.concatenate(records + [zbuf[...].reshape(nz, 128)], axis=0)
    energy, curve = pick(records, S0), pick(records, S1)
    first_step = energy / curve
    delta = first_step - pick(records, GUESS, axis=1)
    weight = by_lane(records.shape, [(Q0, 1.0), (Q1, -2.0 * delta), (Q2, delta * delta)])
    energy_next = jnp.sum(weight * records, keepdims=True)
    weight = by_lane(records.shape, [(E0, 1.0), (E1, -delta), (E2, delta * delta)])
    curve_next = jnp.sum(weight * records, keepdims=True)
    ratio = energy_next / energy
    second_step = energy_next / (curve_next - ratio * energy_next / first_step)
    both = first_step + second_step * (1.0 + ratio)
    back = first_step * second_step
    for i, value in enumerate((first_step, both, back)):
        scal_ref[i] = jnp.broadcast_to(value, block)

    end_halo(0, raw)
    end_halo(1, image_halo)
    to_other(0, z_p, zother).wait_send()
    to_other(1, y_p, yother).wait_send()
    for hop in hops:
        close(*hop).wait_send()
    far_rows(0, nz, lambda row: along_z(row).wait_send())


def finish(cur, z_p, w, y_p, u, scal, drop_hbm, resid_hbm, worst_hbm, drop, resid, worst, sem):
    rows, cols = cur.shape
    pieces = 4
    size = rows // pieces
    wide = [jnp.concatenate([scal[i]] * (cols // 128), axis=1) for i in range(3)]
    copies = []
    for piece in range(pieces):
        for k in range(size // 8):
            at = pl.ds(piece * size + 8 * k, 8)
            below = pl.ds(piece * size + 8 * k + 8, 8)
            z = z_p[below, :]
            new = wide[1] * z - wide[2] * y_p[below, :]
            drop[at, :] = new
            resid[at, :] = cur[at, :] - wide[1] * w[at, :] + wide[2] * u[at, :]
            worst[at, :] = jnp.maximum(wide[0] * z, new)
        part = pl.ds(piece * size, size)
        for i, (src, dst) in enumerate(
            ((drop, drop_hbm), (resid, resid_hbm), (worst, worst_hbm))
        ):
            copy = pltpu.make_async_copy(src.at[part], dst.at[part], sem.at[i, piece])
            copy.start()
            copies.append(copy)
    for copy in copies:
        copy.wait()


def local(nz, nx, nc, current, node_class, class_conductance, pad_mask, via_mask):
    rows, cols = via_mask.shape
    field = jax.ShapeDtypeStruct((rows, cols), jnp.float32)
    tall = jax.ShapeDtypeStruct((rows + 16, cols), jnp.float32)
    full = pltpu.VMEM((rows, cols), jnp.float32)
    whole = pltpu.VMEM((rows, cols), jnp.int32)
    padded = pltpu.VMEM((rows + 16, cols), jnp.float32)
    hbm = pl.BlockSpec(memory_space=pltpu.HBM)
    vmem = pl.BlockSpec(memory_space=pltpu.VMEM)
    dma = pltpu.SemaphoreType.DMA
    scratch = [whole, whole, whole, padded, pltpu.VMEM((4, rows, cols), jnp.float32)]
    scratch += [full] * 5
    near = (2 * REACH + 1, nx * nc)
    scratch += [
        pltpu.VMEM((2, 4, 1, cols), jnp.float32),
        pltpu.VMEM((2, 4, 8, 128), jnp.float32),
        pltpu.VMEM((4, 8, 128), jnp.float32),
    ] * 2
    scratch += [
        pltpu.VMEM((2, 1, cols), jnp.float32),
        pltpu.VMEM((2, 8, 128), jnp.float32),
    ] * 2
    scratch += [
        pltpu.VMEM((1, 128), jnp.float32),
        pltpu.VMEM((*near, 1, 128), jnp.float32),
        pltpu.VMEM((1, 128), jnp.float32),
        pltpu.VMEM((nz, 1, 128), jnp.float32),
        dma((4,)),
        dma((2, 8)),
        dma((2, 8)),
        dma((2,)),
        dma((2,)),
        dma(near),
        dma(near),
        dma((nz,)),
        dma((nz,)),
        pltpu.SemaphoreType.REGULAR,
        pltpu.SemaphoreType.REGULAR,
        pltpu.SemaphoreType.REGULAR((nz,)),
    ]
    limit = 32 * 1024 * 1024
    scalars = jax.ShapeDtypeStruct((3, 8, 128), jnp.float32)
    args = (current[0], node_class[0], class_conductance, pad_mask[0], via_mask)
    stay = [pltpu.with_memory_space_constraint(arg, pltpu.HBM) for arg in args]
    solved = pl.pallas_call(
        functools.partial(kernel, nz, nx, nc),
        out_shape=[field, tall, field, tall, field, scalars],
        in_specs=[hbm, hbm, pl.BlockSpec(memory_space=pltpu.SMEM), hbm, hbm],
        out_specs=[vmem] * 6,
        scratch_shapes=scratch,
        compiler_params=pltpu.CompilerParams(
            collective_id=0, has_side_effects=True, vmem_limit_bytes=limit
        ),
    )(*stay)
    outs = pl.pallas_call(
        finish,
        out_shape=[field] * 3,
        in_specs=[vmem] * 6,
        out_specs=[hbm] * 3,
        scratch_shapes=[full] * 3 + [dma((3, 4))],
        compiler_params=pltpu.CompilerParams(vmem_limit_bytes=limit),
    )(*solved)
    return tuple(out[None] for out in outs)


def solution(mesh):
    grid = P("layer", ("scen", "row"), "col")
    in_specs = (grid, grid, P("layer", None), grid, P(("scen", "row"), "col"))
    sizes = (mesh.shape["row"], mesh.shape["col"], mesh.shape["layer"])
    return jax.shard_map(
        functools.partial(local, *sizes),
        mesh=mesh,
        in_specs=in_specs,
        out_specs=(grid, grid, grid),
        check_vma=False,
    )
```

```python
import functools

import jax
import jax.numpy as jnp
from jax import lax
from jax.experimental import pallas as pl
from jax.experimental.pallas import tpu as pltpu
from jax.sharding import PartitionSpec as P

MESH = pl.DeviceIdType.MESH

via_conductance = 2.0
pad_conductance = 4.0
leakage = 0.05

REACH = 3
PIECES = 4

S0, S1, Q0, Q1, Q2, E0, E1, E2, GUESS = range(9)


def lanes_of(shape):
    return lax.broadcasted_iota(jnp.int32, shape, len(shape) - 1)


def rows_of(shape):
    return lax.broadcasted_iota(jnp.int32, shape, len(shape) - 2)


def pick(record, lane, axis=None):
    kept = jnp.where(lanes_of(record.shape) == lane, record, 0.0)
    return jnp.sum(kept, axis=axis, keepdims=True)


def by_lane(shape, entries):
    lane = lanes_of(shape)
    out = jnp.zeros(shape, jnp.float32)
    for where, value in entries:
        out = jnp.where(lane == where, value, out)
    return out


def fold(value):
    parts = [value[:, i : i + 128] for i in range(0, value.shape[1], 128)]
    while len(parts) > 1:
        parts = [a + b for a, b in zip(parts[::2], parts[1::2])]
    return parts[0]


def kernel(
    nz,
    nx,
    nc,
    cur_hbm,
    cls_hbm,
    cc_hbm,
    pad_hbm,
    via_hbm,
    cur,
    z_p,
    w,
    y_p,
    u,
    scal_ref,
    cc_ref,
    cls,
    pad,
    via,
    cond_p,
    edges,
    coupling,
    base,
    inv,
    zother,
    yother,
    raw_row,
    raw_col,
    raw_corner,
    got_row,
    got_col,
    got_corner,
    y_row,
    y_col,
    goty_row,
    goty_col,
    srec,
    near,
    zrec,
    zbuf,
    in_sem,
    halo_ssem,
    halo_rsem,
    other_ssem,
    other_rsem,
    near_ssem,
    near_rsem,
    z_ssem,
    z_rsem,
    mid_rsem,
    pass_sem,
    low,
    zero_in,
    high,
):
    iz, ix, ic = lax.axis_index("row"), lax.axis_index("col"), lax.axis_index("layer")
    rows, cols = cur.shape
    unroll = 2
    chunks = rows // 8
    reach = REACH
    me = ix * nc + ic

    loads = [
        pltpu.make_async_copy(src, dst, in_sem.at[i])
        for i, (src, dst) in enumerate(
            ((cc_hbm, cc_ref), (cls_hbm, cls), (cur_hbm, cur), (pad_hbm, pad), (via_hbm, via))
        )
    ]
    for copy in loads:
        copy.start()

    for buffer in (got_row, got_col, got_corner, goty_row, goty_col, near, zbuf):
        buffer[...] = jnp.zeros(buffer.shape, jnp.float32)

    def device(dz, dx, dc=0):
        where = {}
        for name, index, size, step in (
            ("row", iz, nz, dz),
            ("col", ix, nx, dx),
            ("layer", ic, nc, dc),
        ):
            if step % size:
                where[name] = lax.rem(index + step % size, size)
        return where

    plane = [(dx, dc) for dx in range(nx) for dc in range(nc)]
    greets = [(0, dx, dc) for dx, dc in plane[1:]]
    greets += [(dz, dx, 0) for dz in (-1, 1) for dx in (0, -1, 1)]
    barrier = pltpu.get_barrier_semaphore()
    for steps in greets:
        pl.semaphore_signal(
            barrier, inc=1, device_id=device(*steps), device_id_type=MESH
        )

    early = max(nz - 5, 2)

    mid_first, mid_stop = max(nz // 4, 2), min(3 * nz // 4, nz - 1 - reach) + 1
    mids = mid_stop - mid_first

    def middle(row):
        return (row >= mid_first) & (row < mid_stop)


    def tell(semaphore, row):
        pl.semaphore_signal(
            semaphore, inc=1, device_id={"row": row}, device_id_type=MESH
        )

    def announce():
        pl.when(iz >= 3)(lambda: pl.semaphore_wait(low, 1))
        pl.when((iz >= 2) & (iz < nz - 1))(lambda: tell(low, iz + 1))

        def one(row, carry):
            tell(high.at[iz], row)
            return carry

        lax.fori_loop(1, iz, one, 0)

    def introduce(row):
        tell(high.at[row], 0)
        pl.when(jnp.logical_not(middle(row)))(lambda: tell(zero_in, row))

    def introduce_early():
        def one(row, carry):
            pl.semaphore_wait(high.at[row], 1)
            introduce(row)
            return carry

        lax.fori_loop(2, early + 1, one, 0)

    def introduce_late():
        pl.semaphore_wait(zero_in, 1)
        tell(high.at[nz - 1], 0)
        for row in range(early + 1, nz - 1):
            introduce(row)

    def meet_all():
        def one(row, carry):
            pl.semaphore_wait(high.at[row], 1)
            return carry

        lax.fori_loop(2, nz, one, 0)

    def meet(row):
        known = jnp.where(iz == 0, nz, jnp.where(iz == 1, early, 0))
        pl.when((row > iz) & (row > known))(lambda: pl.semaphore_wait(high.at[row], 1))
        pl.when((row == 0) & (iz >= 2) & (iz < nz - 1) & jnp.logical_not(middle(iz)))(
            lambda: pl.semaphore_wait(zero_in, 1)
        )

    inside = {
        ("row", -1): iz > 0,
        ("row", 1): iz < nz - 1,
        ("col", -1): ix > 0,
        ("col", 1): ix < nx - 1,
    }

    def exists(dz, dx):
        flags = [inside["row", dz]] if dz else []
        flags += [inside["col", dx]] if dx else []
        return functools.reduce(jnp.logical_and, flags)

    slot = {-1: 0, 1: 1}
    raw = [(dz, 0, raw_row.at[slot[dz]], got_row, slot[-dz]) for dz in (-1, 1)]
    raw += [(0, dx, raw_col.at[slot[dx]], got_col, slot[-dx]) for dx in (-1, 1)]
    raw += [
        (
            dz,
            dx,
            raw_corner.at[2 * slot[dz] + slot[dx]],
            got_corner,
            2 * slot[-dz] + slot[-dx],
        )
        for dz in (-1, 1)
        for dx in (-1, 1)
    ]
    image_halo = [(dz, 0, y_row.at[slot[dz]], goty_row, slot[-dz]) for dz in (-1, 1)]
    image_halo += [(0, dx, y_col.at[slot[dx]], goty_col, slot[-dx]) for dx in (-1, 1)]

    def halo(turn, table, i):
        dz, dx, src, dst, there = table[i]
        return pltpu.make_async_remote_copy(
            src_ref=src,
            dst_ref=dst.at[there],
            send_sem=halo_ssem.at[turn, i],
            recv_sem=halo_rsem.at[turn, i],
            device_id=device(dz, dx),
            device_id_type=MESH,
        )

    def send_halo(turn, table):
        for i, (dz, dx, *_) in enumerate(table):
            pl.when(exists(dz, dx))(halo(turn, table, i).start)

    def take_halo(turn, table):
        for i, (dz, dx, *_) in enumerate(table):
            pl.when(exists(-dz, -dx))(halo(turn, table, i).wait_recv)

    def end_halo(turn, table):
        for i, (dz, dx, *_) in enumerate(table):
            pl.when(exists(dz, dx))(halo(turn, table, i).wait_send)

    pieces = PIECES
    share = rows // pieces

    def to_other(turn, src, dst, piece):
        return pltpu.make_async_remote_copy(
            src_ref=src.at[pl.ds(8 + piece * share, share)],
            dst_ref=dst.at[pl.ds(piece * share, share)],
            send_sem=other_ssem.at[turn, piece],
            recv_sem=other_rsem.at[turn, piece],
            device_id={"layer": 1 - ic},
            device_id_type=MESH,
        )

    def by_piece(body, carry, before=None, after=None):
        for piece in range(pieces):
            if before:
                before(piece)
            first, stop = piece * share // 8, (piece + 1) * share // 8
            carry = lax.fori_loop(first, stop, body, carry, unroll=unroll)
            if after:
                after(piece)
        return carry

    tile = (8, cols)
    block = (8, 128)
    zero = jnp.zeros(block, jnp.float32)
    sub = rows_of(tile)
    narrow_lane = lanes_of(block)

    def at(k, shift=0):
        return pl.ds(pl.multiple_of(8 * k + shift, 8), 8)

    def packed(k, value, left, right):
        here = narrow_lane == k
        left = jnp.where(here, pltpu.roll(value[:, :128], k, 1), left)
        right = jnp.where(here, pltpu.roll(value[:, cols - 128 :], k + 1, 1), right)
        return left, right

    def around(k, prev, here, after, left, right):
        up = pltpu.roll(jnp.where(sub == 7, prev, here), 1, 0)
        down = pltpu.roll(jnp.where(sub == 0, after, here), 7, 0)
        left = pltpu.roll(left, lax.rem(128 - k, 128), 1)
        right = pltpu.roll(right, 127 - k, 1)
        west = pltpu.roll(here, 1, 1)
        west = jnp.concatenate(
            [jnp.where(narrow_lane == 0, left, west[:, :128]), west[:, 128:]], axis=1
        )
        east = pltpu.roll(here, cols - 1, 1)
        east = jnp.concatenate(
            [
                east[:, : cols - 128],
                jnp.where(narrow_lane == 127, right, east[:, cols - 128 :]),
            ],
            axis=1,
        )
        return up, down, west, east

    for copy in loads:
        copy.wait()
    last = cols - 128

    def place(k, value, lane, out):
        moved = pltpu.roll(value, lax.rem(k + 128 - lane, 128), 1)
        return jnp.where(narrow_lane == k, moved, out)

    def node(k, lanes):
        klass = cls[at(k), lanes]
        level = [cc_ref[0, i] for i in range(8)]
        for bit in range(3):
            high_bit = (klass & (1 << bit)) != 0
            level = [jnp.where(high_bit, b, a) for a, b in zip(level[::2], level[1::2])]
        across = via_conductance * via[at(k), lanes].astype(jnp.float32)
        rest = pad_conductance * pad[at(k), lanes].astype(jnp.float32) + leakage
        return level[0], across, across + rest

    def look_up(k, carry):
        cond_p[at(k, 8), :], coupling[at(k), :], base[at(k), :] = node(k, slice(None))
        return carry

    def look_up_ends(k, carry):
        cond, _, rest = node(k, pl.ds(0, 128))
        load = cur[at(k), 0:128]
        borders = [(cond, 0), (cond, 1), (rest, 0), (load, 0)]
        cond, _, rest = node(k, pl.ds(last, 128))
        load = cur[at(k), last:cols]
        borders += [(cond, 127), (cond, 126), (rest, 127), (load, 127)]
        return tuple(place(k, *border, out) for border, out in zip(borders, carry))

    look_up(0, 0)
    look_up(chunks - 1, 0)
    packs = lax.fori_loop(0, chunks, look_up_ends, (zero,) * 8, unroll=4)
    for i in range(8):
        raw_col[i // 4, i % 4] = packs[i]
    for side, row in ((0, 0), (1, rows - 1)):
        inward = 1 - 2 * side
        raw_row[side, 0] = cond_p[8 + row : 9 + row, :]
        raw_row[side, 1] = cond_p[8 + row + inward : 9 + row + inward, :]
        raw_row[side, 2] = base[row : row + 1, :]
        raw_row[side, 3] = cur[row : row + 1, :]
        for end, col in ((0, 0), (1, cols - 1)):
            corner = cond_p[8 + row : 9 + row, col : col + 1]
            raw_corner[2 * side + end] = jnp.broadcast_to(corner, block)

    pl.semaphore_wait(barrier, len(greets))
    send_halo(0, raw)
    announce()
    pl.when(iz == 1)(introduce_early)
    lax.fori_loop(1, chunks - 1, look_up, 0, unroll=unroll)
    take_halo(0, raw)
    pl.when(iz == 0)(lambda: tell(zero_in, nz - 1))
    pl.when(iz == nz - 1)(introduce_late)
    for side, row in ((0, 0), (1, rows + 8)):
        cond_p[row : row + 8, :] = jnp.broadcast_to(got_row[side, 0], tile)

    cond_left, cond_right = got_col[0, 0], got_col[1, 0]

    def edge(here, other):
        return jnp.where(other > 0.0, 0.5 * (here + other), 0.0)

    def precondition(k, energy):
        here = cond_p[at(k, 8), :]
        sides = around(
            k, cond_p[at(k), :], here, cond_p[at(k, 16), :], cond_left, cond_right
        )
        sides = [edge(here, other) for other in sides]
        for i in range(4):
            edges[i, at(k), :] = sides[i]
        diagonal = ((sides[0] + sides[1]) + (sides[2] + sides[3])) + base[at(k), :]
        inverse = 1.0 / diagonal
        resid = cur[at(k), :]
        value = resid * inverse
        inv[at(k), :] = inverse
        z_p[at(k, 8), :] = value
        return energy + fold(resid * value)

    energy = by_piece(
        precondition, zero, after=lambda piece: to_other(0, z_p, zother, piece).start()
    )

    def beyond(here, others, rest, load):
        sides = [edge(here, other) for other in others]
        diagonal = ((sides[0] + sides[1]) + (sides[2] + sides[3])) + rest
        return jnp.where(here > 0.0, load * (1.0 / diagonal), 0.0)

    for side, row, inner in ((0, 0, 8), (1, rows + 8, rows + 7)):
        here, outer, rest, load = [
            jnp.broadcast_to(got_row[side, i], tile) for i in range(4)
        ]
        inner = jnp.broadcast_to(cond_p[inner : inner + 1, :], tile)
        west = pltpu.roll(here, 1, 1)
        west = jnp.concatenate(
            [
                jnp.where(narrow_lane == 0, got_corner[2 * side], west[:, :128]),
                west[:, 128:],
            ],
            axis=1,
        )
        east = pltpu.roll(here, cols - 1, 1)
        east = jnp.concatenate(
            [
                east[:, :last],
                jnp.where(narrow_lane == 127, got_corner[2 * side + 1], east[:, last:]),
            ],
            axis=1,
        )
        z_p[row : row + 8, :] = beyond(here, (outer, inner, west, east), rest, load)

    narrow_sub = rows_of(block)
    z_ends = []
    for side in range(2):
        here, outer, rest, load = [got_col[side, i] for i in range(4)]
        up = pltpu.roll(here, 1, 0)
        up = jnp.where(narrow_sub == 0, pltpu.roll(up, 1, 1), up)
        up = jnp.where((narrow_sub == 0) & (narrow_lane == 0), got_corner[side], up)
        down = pltpu.roll(here, 7, 0)
        down = jnp.where(narrow_sub == 7, pltpu.roll(down, 127, 1), down)
        end = (narrow_sub == 7) & (narrow_lane == chunks - 1)
        down = jnp.where(end, got_corner[2 + side], down)
        inner = raw_col[side, 0]
        z_ends.append(beyond(here, (up, down, outer, inner), rest, load))
    z_left, z_right = z_ends

    def image(k, field, lead, left, right, other):
        values = [field[at(k, 8 * i), :] for i in range(3)]
        sides = around(k, *values, left, right)
        terms = [edges[i, at(k), :] * sides[i] for i in range(4)]
        beside = (terms[0] + terms[1]) + (terms[2] + terms[3])
        return lead - beside - coupling[at(k), :] * other[at(k), :], values[1]

    def first_image(k, carry):
        left, right, curve = carry
        out, value = image(k, z_p, cur[at(k), :], z_left, z_right, zother)
        w[at(k), :] = out
        nxt = out * inv[at(k), :]
        y_p[at(k, 8), :] = nxt
        left, right = packed(k, nxt, left, right)
        return left, right, curve + fold(value * out)

    left, right, curve = by_piece(
        first_image,
        (zero, zero, zero),
        before=lambda piece: to_other(0, z_p, zother, piece).wait_recv(),
        after=lambda piece: to_other(1, y_p, yother, piece).start(),
    )
    y_row[0] = y_p[8:9, :]
    y_row[1] = y_p[rows + 7 : rows + 8, :]
    y_col[0] = left
    y_col[1] = right
    send_halo(1, image_halo)
    energy = jnp.sum(energy, keepdims=True)
    curve = jnp.sum(curve, keepdims=True)
    guess = energy / curve
    pl.when(iz == 0)(meet_all)
    take_halo(1, image_halo)
    for side, row in ((0, 0), (1, rows + 8)):
        y_p[row : row + 8, :] = jnp.broadcast_to(goty_row[side], tile)

    y_left, y_right = goty_col[0], goty_col[1]

    def second_image(k, sums):
        along = w[at(k), :]
        out, nxt = image(k, y_p, along, y_left, y_right, yother)
        u[at(k), :] = out
        left_over = cur[at(k), :] - guess * along
        pre = left_over * inv[at(k), :]
        pre_image = along - guess * out
        terms = (
            left_over * pre,
            left_over * nxt,
            along * nxt,
            pre * pre_image,
            pre * out + nxt * pre_image,
            nxt * out,
        )
        return tuple(a + fold(b) for a, b in zip(sums, terms))

    sums = by_piece(
        second_image,
        (zero,) * 6,
        before=lambda piece: to_other(1, y_p, yother, piece).wait_recv(),
    )

    line = (1, 128)
    entries = [(S0, energy), (S1, curve), (GUESS, guess)]
    entries += [
        (spot, jnp.sum(value, keepdims=True))
        for spot, value in zip((Q0, Q1, Q2, E0, E1, E2), sums)
    ]
    record = by_lane(line, entries)
    srec[...] = record
    near[len(plane) + me] = record

    everyone = range(len(plane))

    def several(ref, first, count, semaphore):
        part = ref.at[pl.ds(first, count)]
        return pltpu.make_async_remote_copy(
            src_ref=part,
            dst_ref=part,
            send_sem=semaphore,
            recv_sem=semaphore,
            device_id=device(1, 0),
            device_id_type=MESH,
        )

    def close(dz, i):
        dx, dc = plane[i]
        where = device(0, dx, dc)
        where["row"] = lax.rem(iz + dz + nz, nz)
        spot = dz + 1
        return pltpu.make_async_remote_copy(
            src_ref=srec,
            dst_ref=near.at[spot * len(plane) + me],
            send_sem=near_ssem.at[spot],
            recv_sem=near_rsem.at[spot],
            device_id=where,
            device_id_type=MESH,
        )

    def close_arrived(spot):
        count = len(plane) - (spot == 1)
        several(near, spot * len(plane), count, near_rsem.at[spot]).wait_recv()

    def greet_plane(dz):
        meet(lax.rem(iz + dz + nz, nz))
        for i in everyone:
            close(dz, i).start()

    def greet_up(dz):
        pl.when(iz + dz >= nz)(lambda: greet_plane(dz))

    def close_left(spot):
        count = len(plane) - (spot == 1)
        several(near, 0, count, near_ssem.at[spot]).wait_send()

    turned = jnp.where(iz >= nz - reach, nz - 1 - iz, 0)
    ups = [1 + lax.rem(i + turned, reach) for i in range(reach)]
    for i in everyone[1:]:
        close(0, i).start()
    for dz in ups:
        greet_up(dz)
    pl.when(iz == 1)(lambda: greet_plane(-1))
    part = pl.ds(mid_first, mids)
    hand_on = pltpu.make_async_remote_copy(
        src_ref=zbuf.at[part],
        dst_ref=zbuf.at[part],
        send_sem=pass_sem,
        recv_sem=mid_rsem,
        device_id={"row": 0},
        device_id_type=MESH,
    )

    def pass_on():
        hand_on.wait_recv()
        hand_on.start()

    pl.when(iz == 1)(pass_on)
    close_arrived(1)

    records = near[pl.ds(len(plane), len(plane))].reshape(len(plane), 128)
    joint = pick(records, S0) / pick(records, S1)
    delta = joint - pick(records, GUESS, axis=1)
    first = by_lane(
        records.shape,
        [(Q0, -2.0 * delta), (Q1, -delta), (E0, -delta), (E1, -2.0 * delta)],
    )
    second = by_lane(records.shape, [(Q0, delta * delta), (E0, delta * delta)])
    records = (
        records
        + first * pltpu.roll(records, 127, 1)
        + second * pltpu.roll(records, 126, 1)
    )
    record = jnp.sum(records, axis=0, keepdims=True)
    record = jnp.where(lanes_of(line) == GUESS, joint, record)
    zrec[...] = record

    def along_z(row, received=z_rsem):
        return pltpu.make_async_remote_copy(
            src_ref=zrec,
            dst_ref=zbuf.at[iz],
            send_sem=z_ssem,
            recv_sem=received,
            device_id={"row": row},
            device_id_type=MESH,
        )

    def direct(source, row):
        near_by = (row + nz - source <= reach) & (row < source)
        return near_by | ((row == 0) & ((source == 1) | middle(source)))

    def far_rows(first, stop, act, leaving=True):
        def one(row, carry):
            pair = (iz, row) if leaving else (row, iz)
            far = (row != iz) & jnp.logical_not(direct(*pair))
            pl.when(far)(lambda: act(row))
            return carry

        lax.fori_loop(first, stop, one, 0)

    def met_send(row):
        meet(row)
        along_z(row).start()

    far_rows(0, jnp.minimum(iz, 1), met_send)
    pl.when(middle(iz))(lambda: along_z(1, mid_rsem).start())
    own = jnp.where(middle(iz), 2, 1)
    far_rows(own, iz, lambda row: along_z(row).start())
    far_rows(iz + 1, nz, met_send)

    end_halo(0, raw)
    end_halo(1, image_halo)
    for piece in range(pieces):
        to_other(0, z_p, zother, piece).wait_send()
        to_other(1, y_p, yother, piece).wait_send()
    close_left(1)
    pl.when(iz == 1)(lambda: close_left(0))
    for step in range(1, reach + 1):
        pl.when(iz + step >= nz)(lambda step=step: close_left(step + 1))

    def wait_far(row, count, receive):
        copies = several(zbuf, 0, count, z_rsem if receive else z_ssem)
        pl.when(row)(copies.wait_recv if receive else copies.wait_send)

    wait_far((iz != 1) & (iz < nz - reach) & jnp.logical_not(middle(iz)), nz - 1, False)
    wait_far(middle(iz), nz - 2, False)
    wait_far(iz == 1, nz - 2, False)
    for step in range(reach):
        wait_far(iz == nz - 1 - step, nz - 1 - reach + step, False)
    wait_far(iz == 0, nz - 2 - reach - mids, True)
    for row in range(1, max(reach, 2)):
        count = nz - 1 - max(reach - row, 0)
        wait_far(iz == row, count - mids * (row == 1), True)
    wait_far(iz >= max(reach, 2), nz - 1, True)
    pl.when(iz == 0)(hand_on.wait_recv)
    pl.when(iz == 1)(hand_on.wait_send)
    pl.when(iz == 0)(lambda: close_arrived(0))
    for step in range(reach, 0, -1):
        pl.when(iz < step)(lambda step=step: close_arrived(step + 1))

    records = [near[...].reshape(near.shape[0], 128), zbuf[...].reshape(nz, 128)]
    records = jnp.concatenate(records, axis=0)
    energy, curve = pick(records, S0), pick(records, S1)
    first_step = energy / curve
    delta = first_step - pick(records, GUESS, axis=1)
    weight = by_lane(records.shape, [(Q0, 1.0), (Q1, -2.0 * delta), (Q2, delta * delta)])
    energy_next = jnp.sum(weight * records, keepdims=True)
    weight = by_lane(records.shape, [(E0, 1.0), (E1, -delta), (E2, delta * delta)])
    curve_next = jnp.sum(weight * records, keepdims=True)
    ratio = energy_next / energy
    second_step = energy_next / (curve_next - ratio * energy_next / first_step)
    both = first_step + second_step * (1.0 + ratio)
    back = first_step * second_step
    for i, value in enumerate((first_step, both, back)):
        scal_ref[i] = jnp.broadcast_to(value, block)


def finish(cur, z_p, w, y_p, u, scal, drop_hbm, resid_hbm, worst_hbm, drop, resid, worst, sem):
    rows, cols = cur.shape
    pieces = 4
    size = rows // pieces
    wide = [jnp.concatenate([scal[i]] * (cols // 128), axis=1) for i in range(3)]
    copies = []
    for piece in range(pieces):
        for k in range(size // 8):
            at = pl.ds(piece * size + 8 * k, 8)
            below = pl.ds(piece * size + 8 * k + 8, 8)
            z = z_p[below, :]
            new = wide[1] * z - wide[2] * y_p[below, :]
            drop[at, :] = new
            resid[at, :] = cur[at, :] - wide[1] * w[at, :] + wide[2] * u[at, :]
            worst[at, :] = jnp.maximum(wide[0] * z, new)
        part = pl.ds(piece * size, size)
        for i, (src, dst) in enumerate(
            ((drop, drop_hbm), (resid, resid_hbm), (worst, worst_hbm))
        ):
            copy = pltpu.make_async_copy(src.at[part], dst.at[part], sem.at[i, piece])
            copy.start()
            copies.append(copy)
    for copy in copies:
        copy.wait()


def local(nz, nx, nc, current, node_class, class_conductance, pad_mask, via_mask):
    rows, cols = via_mask.shape
    field = jax.ShapeDtypeStruct((rows, cols), jnp.float32)
    tall = jax.ShapeDtypeStruct((rows + 16, cols), jnp.float32)
    full = pltpu.VMEM((rows, cols), jnp.float32)
    whole = pltpu.VMEM((rows, cols), jnp.int32)
    padded = pltpu.VMEM((rows + 16, cols), jnp.float32)
    hbm = pl.BlockSpec(memory_space=pltpu.HBM)
    vmem = pl.BlockSpec(memory_space=pltpu.VMEM)
    dma = pltpu.SemaphoreType.DMA
    scratch = [pltpu.SMEM(class_conductance.shape, jnp.float32)]
    scratch += [whole, whole, whole, padded, pltpu.VMEM((4, rows, cols), jnp.float32)]
    scratch += [full] * 5
    near = (REACH + 2) * nx * nc
    scratch += [
        pltpu.VMEM((2, 4, 1, cols), jnp.float32),
        pltpu.VMEM((2, 4, 8, 128), jnp.float32),
        pltpu.VMEM((4, 8, 128), jnp.float32),
    ] * 2
    scratch += [
        pltpu.VMEM((2, 1, cols), jnp.float32),
        pltpu.VMEM((2, 8, 128), jnp.float32),
    ] * 2
    scratch += [
        pltpu.VMEM((1, 128), jnp.float32),
        pltpu.VMEM((near, 1, 128), jnp.float32),
        pltpu.VMEM((1, 128), jnp.float32),
        pltpu.VMEM((nz, 1, 128), jnp.float32),
        dma((5,)),
        dma((2, 8)),
        dma((2, 8)),
        dma((2, PIECES)),
        dma((2, PIECES)),
        dma((REACH + 2,)),
        dma((REACH + 2,)),
        dma,
        dma,
        dma,
        dma,
        pltpu.SemaphoreType.REGULAR,
        pltpu.SemaphoreType.REGULAR,
        pltpu.SemaphoreType.REGULAR((nz,)),
    ]
    limit = 32 * 1024 * 1024
    scalars = jax.ShapeDtypeStruct((3, 8, 128), jnp.float32)
    args = (current[0], node_class[0], class_conductance, pad_mask[0], via_mask)
    stay = [pltpu.with_memory_space_constraint(arg, pltpu.HBM) for arg in args]
    solved = pl.pallas_call(
        functools.partial(kernel, nz, nx, nc),
        out_shape=[field, tall, field, tall, field, scalars],
        in_specs=[hbm] * 5,
        out_specs=[vmem] * 6,
        scratch_shapes=scratch,
        compiler_params=pltpu.CompilerParams(
            collective_id=0, has_side_effects=True, vmem_limit_bytes=limit
        ),
    )(*stay)
    outs = pl.pallas_call(
        finish,
        out_shape=[field] * 3,
        in_specs=[vmem] * 6,
        out_specs=[hbm] * 3,
        scratch_shapes=[full] * 3 + [dma((3, 4))],
        compiler_params=pltpu.CompilerParams(vmem_limit_bytes=limit),
    )(*solved)
    return tuple(out[None] for out in outs)


def solution(mesh):
    grid = P("layer", ("scen", "row"), "col")
    in_specs = (grid, grid, P("layer", None), grid, P(("scen", "row"), "col"))
    sizes = (mesh.shape["row"], mesh.shape["col"], mesh.shape["layer"])
    return jax.shard_map(
        functools.partial(local, *sizes),
        mesh=mesh,
        in_specs=in_specs,
        out_specs=(grid, grid, grid),
        check_vma=False,
    )
```

```python
import functools

import jax
import jax.numpy as jnp
from jax import lax
from jax.experimental import pallas as pl
from jax.experimental.pallas import tpu as pltpu
from jax.sharding import PartitionSpec as P

MESH = pl.DeviceIdType.MESH

via_conductance = 2.0
pad_conductance = 4.0
leakage = 0.05

REACH = 2
PIECES = 4

S0, S1, Q0, Q1, Q2, E0, E1, E2, GUESS = range(9)


def lanes_of(shape):
    return lax.broadcasted_iota(jnp.int32, shape, len(shape) - 1)


def rows_of(shape):
    return lax.broadcasted_iota(jnp.int32, shape, len(shape) - 2)


def pick(record, lane, axis=None):
    kept = jnp.where(lanes_of(record.shape) == lane, record, 0.0)
    return jnp.sum(kept, axis=axis, keepdims=True)


def by_lane(shape, entries):
    lane = lanes_of(shape)
    out = jnp.zeros(shape, jnp.float32)
    for where, value in entries:
        out = jnp.where(lane == where, value, out)
    return out


def fold(value):
    parts = [value[:, i : i + 128] for i in range(0, value.shape[1], 128)]
    while len(parts) > 1:
        parts = [a + b for a, b in zip(parts[::2], parts[1::2])]
    return parts[0]


def kernel(
    nz,
    nx,
    nc,
    cur_hbm,
    cls_hbm,
    cc_hbm,
    pad_hbm,
    via_hbm,
    cur,
    z_p,
    w,
    y_p,
    u,
    scal_ref,
    cc_ref,
    cls,
    pad,
    via,
    cond_p,
    edges,
    coupling,
    base,
    inv,
    zother,
    yother,
    raw_row,
    raw_col,
    raw_corner,
    got_row,
    got_col,
    got_corner,
    y_row,
    y_col,
    goty_row,
    goty_col,
    srec,
    near,
    zrec,
    zbuf,
    in_sem,
    halo_ssem,
    halo_rsem,
    other_ssem,
    other_rsem,
    near_ssem,
    near_rsem,
    z_ssem,
    z_rsem,
    mid_rsem,
    pass_sem,
    low,
    zero_in,
    high,
):
    iz, ix, ic = lax.axis_index("row"), lax.axis_index("col"), lax.axis_index("layer")
    rows, cols = cur.shape
    unroll = 4
    chunks = rows // 8
    reach = REACH
    me = ix * nc + ic

    loads = [
        pltpu.make_async_copy(src, dst, in_sem.at[i])
        for i, (src, dst) in enumerate(
            ((cc_hbm, cc_ref), (cls_hbm, cls), (cur_hbm, cur), (pad_hbm, pad), (via_hbm, via))
        )
    ]
    for copy in loads:
        copy.start()

    for buffer in (got_row, got_col, got_corner, goty_row, goty_col, near, zbuf):
        buffer[...] = jnp.zeros(buffer.shape, jnp.float32)

    def device(dz, dx, dc=0):
        where = {}
        for name, index, size, step in (
            ("row", iz, nz, dz),
            ("col", ix, nx, dx),
            ("layer", ic, nc, dc),
        ):
            if step % size:
                where[name] = lax.rem(index + step % size, size)
        return where

    plane = [(dx, dc) for dx in range(nx) for dc in range(nc)]
    greets = [(0, dx, dc) for dx, dc in plane[1:]]
    greets += [(dz, dx, 0) for dz in (-1, 1) for dx in (0, -1, 1)]
    barrier = pltpu.get_barrier_semaphore()
    for steps in greets:
        pl.semaphore_signal(
            barrier, inc=1, device_id=device(*steps), device_id_type=MESH
        )

    early = max(nz - 5, 2)

    mid_first, mid_stop = max(nz // 4, 2), min(3 * nz // 4, nz - 1 - reach) + 1
    mids = mid_stop - mid_first

    def middle(row):
        return (row >= mid_first) & (row < mid_stop)


    def tell(semaphore, row):
        pl.semaphore_signal(
            semaphore, inc=1, device_id={"row": row}, device_id_type=MESH
        )

    def announce():
        pl.when(iz >= 3)(lambda: pl.semaphore_wait(low, 1))
        pl.when((iz >= 2) & (iz < nz - 1))(lambda: tell(low, iz + 1))

        def one(row, carry):
            tell(high.at[iz], row)
            return carry

        lax.fori_loop(1, iz, one, 0)

    def introduce(row):
        tell(high.at[row], 0)
        pl.when(jnp.logical_not(middle(row)))(lambda: tell(zero_in, row))

    def introduce_early():
        def one(row, carry):
            pl.semaphore_wait(high.at[row], 1)
            introduce(row)
            return carry

        lax.fori_loop(2, early + 1, one, 0)

    def introduce_late():
        pl.semaphore_wait(zero_in, 1)
        tell(high.at[nz - 1], 0)
        for row in range(early + 1, nz - 1):
            introduce(row)

    def meet_all():
        def one(row, carry):
            pl.semaphore_wait(high.at[row], 1)
            return carry

        lax.fori_loop(2, nz, one, 0)

    def meet(row):
        known = jnp.where(iz == 0, nz, jnp.where(iz == 1, early, 0))
        pl.when((row > iz) & (row > known))(lambda: pl.semaphore_wait(high.at[row], 1))
        pl.when((row == 0) & (iz >= 2) & (iz < nz - 1) & jnp.logical_not(middle(iz)))(
            lambda: pl.semaphore_wait(zero_in, 1)
        )

    inside = {
        ("row", -1): iz > 0,
        ("row", 1): iz < nz - 1,
        ("col", -1): ix > 0,
        ("col", 1): ix < nx - 1,
    }

    def exists(dz, dx):
        flags = [inside["row", dz]] if dz else []
        flags += [inside["col", dx]] if dx else []
        return functools.reduce(jnp.logical_and, flags)

    slot = {-1: 0, 1: 1}
    raw = [(dz, 0, raw_row.at[slot[dz]], got_row, slot[-dz]) for dz in (-1, 1)]
    raw += [(0, dx, raw_col.at[slot[dx]], got_col, slot[-dx]) for dx in (-1, 1)]
    raw += [
        (
            dz,
            dx,
            raw_corner.at[2 * slot[dz] + slot[dx]],
            got_corner,
            2 * slot[-dz] + slot[-dx],
        )
        for dz in (-1, 1)
        for dx in (-1, 1)
    ]
    image_halo = [(dz, 0, y_row.at[slot[dz]], goty_row, slot[-dz]) for dz in (-1, 1)]
    image_halo += [(0, dx, y_col.at[slot[dx]], goty_col, slot[-dx]) for dx in (-1, 1)]

    def halo(turn, table, i):
        dz, dx, src, dst, there = table[i]
        return pltpu.make_async_remote_copy(
            src_ref=src,
            dst_ref=dst.at[there],
            send_sem=halo_ssem.at[turn, i],
            recv_sem=halo_rsem.at[turn, i],
            device_id=device(dz, dx),
            device_id_type=MESH,
        )

    def send_halo(turn, table):
        for i, (dz, dx, *_) in enumerate(table):
            pl.when(exists(dz, dx))(halo(turn, table, i).start)

    def take_halo(turn, table):
        for i, (dz, dx, *_) in enumerate(table):
            pl.when(exists(-dz, -dx))(halo(turn, table, i).wait_recv)

    def end_halo(turn, table):
        for i, (dz, dx, *_) in enumerate(table):
            pl.when(exists(dz, dx))(halo(turn, table, i).wait_send)

    pieces = PIECES
    share = rows // pieces

    def to_other(turn, src, dst, piece):
        return pltpu.make_async_remote_copy(
            src_ref=src.at[pl.ds(8 + piece * share, share)],
            dst_ref=dst.at[pl.ds(piece * share, share)],
            send_sem=other_ssem.at[turn, piece],
            recv_sem=other_rsem.at[turn, piece],
            device_id={"layer": 1 - ic},
            device_id_type=MESH,
        )

    def by_piece(body, carry, before=None, after=None):
        for piece in range(pieces):
            if before:
                before(piece)
            first, stop = piece * share // 8, (piece + 1) * share // 8
            carry = lax.fori_loop(first, stop, body, carry, unroll=unroll)
            if after:
                after(piece)
        return carry

    tile = (8, cols)
    block = (8, 128)
    zero = jnp.zeros(block, jnp.float32)
    sub = rows_of(tile)
    narrow_lane = lanes_of(block)

    def at(k, shift=0):
        return pl.ds(pl.multiple_of(8 * k + shift, 8), 8)

    def packed(k, value, left, right):
        here = narrow_lane == k
        left = jnp.where(here, pltpu.roll(value[:, :128], k, 1), left)
        right = jnp.where(here, pltpu.roll(value[:, cols - 128 :], k + 1, 1), right)
        return left, right

    def around(k, prev, here, after, left, right):
        up = pltpu.roll(jnp.where(sub == 7, prev, here), 1, 0)
        down = pltpu.roll(jnp.where(sub == 0, after, here), 7, 0)
        left = pltpu.roll(left, lax.rem(128 - k, 128), 1)
        right = pltpu.roll(right, 127 - k, 1)
        west = pltpu.roll(here, 1, 1)
        west = jnp.concatenate(
            [jnp.where(narrow_lane == 0, left, west[:, :128]), west[:, 128:]], axis=1
        )
        east = pltpu.roll(here, cols - 1, 1)
        east = jnp.concatenate(
            [
                east[:, : cols - 128],
                jnp.where(narrow_lane == 127, right, east[:, cols - 128 :]),
            ],
            axis=1,
        )
        return up, down, west, east

    for copy in loads:
        copy.wait()
    last = cols - 128

    def place(k, value, lane, out):
        moved = pltpu.roll(value, lax.rem(k + 128 - lane, 128), 1)
        return jnp.where(narrow_lane == k, moved, out)

    def node(k, lanes):
        klass = cls[at(k), lanes]
        level = [cc_ref[0, i] for i in range(8)]
        for bit in range(3):
            high_bit = (klass & (1 << bit)) != 0
            level = [jnp.where(high_bit, b, a) for a, b in zip(level[::2], level[1::2])]
        across = via_conductance * via[at(k), lanes].astype(jnp.float32)
        rest = pad_conductance * pad[at(k), lanes].astype(jnp.float32) + leakage
        return level[0], across, across + rest

    def look_up(k, carry):
        cond_p[at(k, 8), :], coupling[at(k), :], base[at(k), :] = node(k, slice(None))
        return carry

    def look_up_ends(k, carry):
        cond, _, rest = node(k, pl.ds(0, 128))
        load = cur[at(k), 0:128]
        borders = [(cond, 0), (cond, 1), (rest, 0), (load, 0)]
        cond, _, rest = node(k, pl.ds(last, 128))
        load = cur[at(k), last:cols]
        borders += [(cond, 127), (cond, 126), (rest, 127), (load, 127)]
        return tuple(place(k, *border, out) for border, out in zip(borders, carry))

    look_up(0, 0)
    look_up(chunks - 1, 0)
    packs = lax.fori_loop(0, chunks, look_up_ends, (zero,) * 8, unroll=4)
    for i in range(8):
        raw_col[i // 4, i % 4] = packs[i]
    for side, row in ((0, 0), (1, rows - 1)):
        inward = 1 - 2 * side
        raw_row[side, 0] = cond_p[8 + row : 9 + row, :]
        raw_row[side, 1] = cond_p[8 + row + inward : 9 + row + inward, :]
        raw_row[side, 2] = base[row : row + 1, :]
        raw_row[side, 3] = cur[row : row + 1, :]
        for end, col in ((0, 0), (1, cols - 1)):
            corner = cond_p[8 + row : 9 + row, col : col + 1]
            raw_corner[2 * side + end] = jnp.broadcast_to(corner, block)

    pl.semaphore_wait(barrier, len(greets))
    send_halo(0, raw)
    announce()
    pl.when(iz == 1)(introduce_early)
    lax.fori_loop(1, chunks - 1, look_up, 0, unroll=unroll)
    take_halo(0, raw)
    pl.when(iz == 0)(lambda: tell(zero_in, nz - 1))
    pl.when(iz == nz - 1)(introduce_late)
    for side, row in ((0, 0), (1, rows + 8)):
        cond_p[row : row + 8, :] = jnp.broadcast_to(got_row[side, 0], tile)

    cond_left, cond_right = got_col[0, 0], got_col[1, 0]

    def edge(here, other):
        return jnp.where(other > 0.0, 0.5 * (here + other), 0.0)

    def precondition(k, energy):
        here = cond_p[at(k, 8), :]
        sides = around(
            k, cond_p[at(k), :], here, cond_p[at(k, 16), :], cond_left, cond_right
        )
        sides = [edge(here, other) for other in sides]
        for i in range(4):
            edges[i, at(k), :] = sides[i]
        diagonal = ((sides[0] + sides[1]) + (sides[2] + sides[3])) + base[at(k), :]
        inverse = 1.0 / diagonal
        resid = cur[at(k), :]
        value = resid * inverse
        inv[at(k), :] = inverse
        z_p[at(k, 8), :] = value
        return energy + fold(resid * value)

    energy = by_piece(
        precondition, zero, after=lambda piece: to_other(0, z_p, zother, piece).start()
    )

    def beyond(here, others, rest, load):
        sides = [edge(here, other) for other in others]
        diagonal = ((sides[0] + sides[1]) + (sides[2] + sides[3])) + rest
        return jnp.where(here > 0.0, load * (1.0 / diagonal), 0.0)

    for side, row, inner in ((0, 0, 8), (1, rows + 8, rows + 7)):
        here, outer, rest, load = [
            jnp.broadcast_to(got_row[side, i], tile) for i in range(4)
        ]
        inner = jnp.broadcast_to(cond_p[inner : inner + 1, :], tile)
        west = pltpu.roll(here, 1, 1)
        west = jnp.concatenate(
            [
                jnp.where(narrow_lane == 0, got_corner[2 * side], west[:, :128]),
                west[:, 128:],
            ],
            axis=1,
        )
        east = pltpu.roll(here, cols - 1, 1)
        east = jnp.concatenate(
            [
                east[:, :last],
                jnp.where(narrow_lane == 127, got_corner[2 * side + 1], east[:, last:]),
            ],
            axis=1,
        )
        z_p[row : row + 8, :] = beyond(here, (outer, inner, west, east), rest, load)

    narrow_sub = rows_of(block)
    z_ends = []
    for side in range(2):
        here, outer, rest, load = [got_col[side, i] for i in range(4)]
        up = pltpu.roll(here, 1, 0)
        up = jnp.where(narrow_sub == 0, pltpu.roll(up, 1, 1), up)
        up = jnp.where((narrow_sub == 0) & (narrow_lane == 0), got_corner[side], up)
        down = pltpu.roll(here, 7, 0)
        down = jnp.where(narrow_sub == 7, pltpu.roll(down, 127, 1), down)
        end = (narrow_sub == 7) & (narrow_lane == chunks - 1)
        down = jnp.where(end, got_corner[2 + side], down)
        inner = raw_col[side, 0]
        z_ends.append(beyond(here, (up, down, outer, inner), rest, load))
    z_left, z_right = z_ends

    def image(k, field, lead, left, right, other):
        values = [field[at(k, 8 * i), :] for i in range(3)]
        sides = around(k, *values, left, right)
        terms = [edges[i, at(k), :] * sides[i] for i in range(4)]
        beside = (terms[0] + terms[1]) + (terms[2] + terms[3])
        return lead - beside - coupling[at(k), :] * other[at(k), :], values[1]

    def first_image(k, carry):
        left, right, curve = carry
        out, value = image(k, z_p, cur[at(k), :], z_left, z_right, zother)
        w[at(k), :] = out
        nxt = out * inv[at(k), :]
        y_p[at(k, 8), :] = nxt
        left, right = packed(k, nxt, left, right)
        return left, right, curve + fold(value * out)

    left, right, curve = by_piece(
        first_image,
        (zero, zero, zero),
        before=lambda piece: to_other(0, z_p, zother, piece).wait_recv(),
        after=lambda piece: to_other(1, y_p, yother, piece).start(),
    )
    y_row[0] = y_p[8:9, :]
    y_row[1] = y_p[rows + 7 : rows + 8, :]
    y_col[0] = left
    y_col[1] = right
    send_halo(1, image_halo)
    energy = jnp.sum(energy, keepdims=True)
    curve = jnp.sum(curve, keepdims=True)
    guess = energy / curve
    pl.when(iz == 0)(meet_all)
    take_halo(1, image_halo)
    for side, row in ((0, 0), (1, rows + 8)):
        y_p[row : row + 8, :] = jnp.broadcast_to(goty_row[side], tile)

    y_left, y_right = goty_col[0], goty_col[1]

    def second_image(k, sums):
        along = w[at(k), :]
        out, nxt = image(k, y_p, along, y_left, y_right, yother)
        u[at(k), :] = out
        left_over = cur[at(k), :] - guess * along
        pre = left_over * inv[at(k), :]
        pre_image = along - guess * out
        terms = (
            left_over * pre,
            left_over * nxt,
            along * nxt,
            pre * pre_image,
            pre * out + nxt * pre_image,
            nxt * out,
        )
        return tuple(a + fold(b) for a, b in zip(sums, terms))

    sums = by_piece(
        second_image,
        (zero,) * 6,
        before=lambda piece: to_other(1, y_p, yother, piece).wait_recv(),
    )

    line = (1, 128)
    entries = [(S0, energy), (S1, curve), (GUESS, guess)]
    entries += [
        (spot, jnp.sum(value, keepdims=True))
        for spot, value in zip((Q0, Q1, Q2, E0, E1, E2), sums)
    ]
    record = by_lane(line, entries)
    srec[...] = record
    near[len(plane) + me] = record

    everyone = range(len(plane))

    def several(ref, first, count, semaphore):
        part = ref.at[pl.ds(first, count)]
        return pltpu.make_async_remote_copy(
            src_ref=part,
            dst_ref=part,
            send_sem=semaphore,
            recv_sem=semaphore,
            device_id=device(1, 0),
            device_id_type=MESH,
        )

    def close(dz, i):
        dx, dc = plane[i]
        where = device(0, dx, dc)
        where["row"] = lax.rem(iz + dz + nz, nz)
        spot = dz + 1
        return pltpu.make_async_remote_copy(
            src_ref=srec,
            dst_ref=near.at[spot * len(plane) + me],
            send_sem=near_ssem.at[spot],
            recv_sem=near_rsem.at[spot],
            device_id=where,
            device_id_type=MESH,
        )

    def close_arrived(spot):
        count = len(plane) - (spot == 1)
        several(near, spot * len(plane), count, near_rsem.at[spot]).wait_recv()

    def greet_plane(dz):
        meet(lax.rem(iz + dz + nz, nz))
        for i in everyone:
            close(dz, i).start()

    def greet_up(dz):
        pl.when(iz + dz >= nz)(lambda: greet_plane(dz))

    def close_left(spot):
        count = len(plane) - (spot == 1)
        several(near, 0, count, near_ssem.at[spot]).wait_send()

    turned = jnp.where(iz >= nz - reach, nz - 1 - iz, 0)
    ups = [1 + lax.rem(i + turned, reach) for i in range(reach)]
    for i in everyone[1:]:
        close(0, i).start()
    for dz in ups:
        greet_up(dz)
    pl.when(iz == 1)(lambda: greet_plane(-1))
    part = pl.ds(mid_first, mids)
    hand_on = pltpu.make_async_remote_copy(
        src_ref=zbuf.at[part],
        dst_ref=zbuf.at[part],
        send_sem=pass_sem,
        recv_sem=mid_rsem,
        device_id={"row": 0},
        device_id_type=MESH,
    )

    def pass_on():
        hand_on.wait_recv()
        hand_on.start()

    pl.when(iz == 1)(pass_on)
    close_arrived(1)

    records = near[pl.ds(len(plane), len(plane))].reshape(len(plane), 128)
    joint = pick(records, S0) / pick(records, S1)
    delta = joint - pick(records, GUESS, axis=1)
    first = by_lane(
        records.shape,
        [(Q0, -2.0 * delta), (Q1, -delta), (E0, -delta), (E1, -2.0 * delta)],
    )
    second = by_lane(records.shape, [(Q0, delta * delta), (E0, delta * delta)])
    records = (
        records
        + first * pltpu.roll(records, 127, 1)
        + second * pltpu.roll(records, 126, 1)
    )
    record = jnp.sum(records, axis=0, keepdims=True)
    record = jnp.where(lanes_of(line) == GUESS, joint, record)
    zrec[...] = record

    def along_z(row, received=z_rsem):
        return pltpu.make_async_remote_copy(
            src_ref=zrec,
            dst_ref=zbuf.at[iz],
            send_sem=z_ssem,
            recv_sem=received,
            device_id={"row": row},
            device_id_type=MESH,
        )

    def direct(source, row):
        near_by = (row + nz - source <= reach) & (row < source)
        return near_by | ((row == 0) & ((source == 1) | middle(source)))

    def far_rows(first, stop, act, leaving=True):
        def one(row, carry):
            pair = (iz, row) if leaving else (row, iz)
            far = (row != iz) & jnp.logical_not(direct(*pair))
            pl.when(far)(lambda: act(row))
            return carry

        lax.fori_loop(first, stop, one, 0)

    def met_send(row):
        meet(row)
        along_z(row).start()

    far_rows(0, jnp.minimum(iz, 1), met_send)
    pl.when(middle(iz))(lambda: along_z(1, mid_rsem).start())
    own = jnp.where(middle(iz), 2, 1)
    far_rows(own, iz, lambda row: along_z(row).start())
    far_rows(iz + 1, nz, met_send)

    end_halo(0, raw)
    end_halo(1, image_halo)
    for piece in range(pieces):
        to_other(0, z_p, zother, piece).wait_send()
        to_other(1, y_p, yother, piece).wait_send()
    close_left(1)
    pl.when(iz == 1)(lambda: close_left(0))
    for step in range(1, reach + 1):
        pl.when(iz + step >= nz)(lambda step=step: close_left(step + 1))

    def wait_far(row, count, receive):
        copies = several(zbuf, 0, count, z_rsem if receive else z_ssem)
        pl.when(row)(copies.wait_recv if receive else copies.wait_send)

    wait_far((iz != 1) & (iz < nz - reach) & jnp.logical_not(middle(iz)), nz - 1, False)
    wait_far(middle(iz), nz - 2, False)
    wait_far(iz == 1, nz - 2, False)
    for step in range(reach):
        wait_far(iz == nz - 1 - step, nz - 1 - reach + step, False)
    wait_far(iz == 0, nz - 2 - reach - mids, True)
    for row in range(1, max(reach, 2)):
        count = nz - 1 - max(reach - row, 0)
        wait_far(iz == row, count - mids * (row == 1), True)
    wait_far(iz >= max(reach, 2), nz - 1, True)
    pl.when(iz == 0)(hand_on.wait_recv)
    pl.when(iz == 1)(hand_on.wait_send)
    pl.when(iz == 0)(lambda: close_arrived(0))
    for step in range(reach, 0, -1):
        pl.when(iz < step)(lambda step=step: close_arrived(step + 1))

    records = [near[...].reshape(near.shape[0], 128), zbuf[...].reshape(nz, 128)]
    records = jnp.concatenate(records, axis=0)
    energy, curve = pick(records, S0), pick(records, S1)
    first_step = energy / curve
    delta = first_step - pick(records, GUESS, axis=1)
    weight = by_lane(records.shape, [(Q0, 1.0), (Q1, -2.0 * delta), (Q2, delta * delta)])
    energy_next = jnp.sum(weight * records, keepdims=True)
    weight = by_lane(records.shape, [(E0, 1.0), (E1, -delta), (E2, delta * delta)])
    curve_next = jnp.sum(weight * records, keepdims=True)
    ratio = energy_next / energy
    second_step = energy_next / (curve_next - ratio * energy_next / first_step)
    both = first_step + second_step * (1.0 + ratio)
    back = first_step * second_step
    for i, value in enumerate((first_step, both, back)):
        scal_ref[i] = jnp.broadcast_to(value, block)


def finish(cur, z_p, w, y_p, u, scal, drop_hbm, resid_hbm, worst_hbm, drop, resid, worst, sem):
    rows, cols = cur.shape
    pieces = 4
    size = rows // pieces
    wide = [jnp.concatenate([scal[i]] * (cols // 128), axis=1) for i in range(3)]
    copies = []
    for piece in range(pieces):
        for k in range(size // 8):
            at = pl.ds(piece * size + 8 * k, 8)
            below = pl.ds(piece * size + 8 * k + 8, 8)
            z = z_p[below, :]
            new = wide[1] * z - wide[2] * y_p[below, :]
            drop[at, :] = new
            resid[at, :] = cur[at, :] - wide[1] * w[at, :] + wide[2] * u[at, :]
            worst[at, :] = jnp.maximum(wide[0] * z, new)
        part = pl.ds(piece * size, size)
        for i, (src, dst) in enumerate(
            ((drop, drop_hbm), (resid, resid_hbm), (worst, worst_hbm))
        ):
            copy = pltpu.make_async_copy(src.at[part], dst.at[part], sem.at[i, piece])
            copy.start()
            copies.append(copy)
    for copy in copies:
        copy.wait()


def local(nz, nx, nc, current, node_class, class_conductance, pad_mask, via_mask):
    rows, cols = via_mask.shape
    field = jax.ShapeDtypeStruct((rows, cols), jnp.float32)
    tall = jax.ShapeDtypeStruct((rows + 16, cols), jnp.float32)
    full = pltpu.VMEM((rows, cols), jnp.float32)
    whole = pltpu.VMEM((rows, cols), jnp.int32)
    padded = pltpu.VMEM((rows + 16, cols), jnp.float32)
    hbm = pl.BlockSpec(memory_space=pltpu.HBM)
    vmem = pl.BlockSpec(memory_space=pltpu.VMEM)
    dma = pltpu.SemaphoreType.DMA
    scratch = [pltpu.SMEM(class_conductance.shape, jnp.float32)]
    scratch += [whole, whole, whole, padded, pltpu.VMEM((4, rows, cols), jnp.float32)]
    scratch += [full] * 5
    near = (REACH + 2) * nx * nc
    scratch += [
        pltpu.VMEM((2, 4, 1, cols), jnp.float32),
        pltpu.VMEM((2, 4, 8, 128), jnp.float32),
        pltpu.VMEM((4, 8, 128), jnp.float32),
    ] * 2
    scratch += [
        pltpu.VMEM((2, 1, cols), jnp.float32),
        pltpu.VMEM((2, 8, 128), jnp.float32),
    ] * 2
    scratch += [
        pltpu.VMEM((1, 128), jnp.float32),
        pltpu.VMEM((near, 1, 128), jnp.float32),
        pltpu.VMEM((1, 128), jnp.float32),
        pltpu.VMEM((nz, 1, 128), jnp.float32),
        dma((5,)),
        dma((2, 8)),
        dma((2, 8)),
        dma((2, PIECES)),
        dma((2, PIECES)),
        dma((REACH + 2,)),
        dma((REACH + 2,)),
        dma,
        dma,
        dma,
        dma,
        pltpu.SemaphoreType.REGULAR,
        pltpu.SemaphoreType.REGULAR,
        pltpu.SemaphoreType.REGULAR((nz,)),
    ]
    limit = 32 * 1024 * 1024
    scalars = jax.ShapeDtypeStruct((3, 8, 128), jnp.float32)
    args = (current[0], node_class[0], class_conductance, pad_mask[0], via_mask)
    stay = [pltpu.with_memory_space_constraint(arg, pltpu.HBM) for arg in args]
    solved = pl.pallas_call(
        functools.partial(kernel, nz, nx, nc),
        out_shape=[field, tall, field, tall, field, scalars],
        in_specs=[hbm] * 5,
        out_specs=[vmem] * 6,
        scratch_shapes=scratch,
        compiler_params=pltpu.CompilerParams(
            collective_id=0, has_side_effects=True, vmem_limit_bytes=limit
        ),
    )(*stay)
    outs = pl.pallas_call(
        finish,
        out_shape=[field] * 3,
        in_specs=[vmem] * 6,
        out_specs=[hbm] * 3,
        scratch_shapes=[full] * 3 + [dma((3, 4))],
        compiler_params=pltpu.CompilerParams(vmem_limit_bytes=limit),
    )(*solved)
    return tuple(out[None] for out in outs)


def solution(mesh):
    grid = P("layer", ("scen", "row"), "col")
    in_specs = (grid, grid, P("layer", None), grid, P(("scen", "row"), "col"))
    sizes = (mesh.shape["row"], mesh.shape["col"], mesh.shape["layer"])
    return jax.shard_map(
        functools.partial(local, *sizes),
        mesh=mesh,
        in_specs=in_specs,
        out_specs=(grid, grid, grid),
        check_vma=False,
    )
```

```python
import functools

import jax
import jax.numpy as jnp
from jax import lax
from jax.experimental import pallas as pl
from jax.experimental.pallas import tpu as pltpu
from jax.sharding import PartitionSpec as P

MESH = pl.DeviceIdType.MESH

via_conductance = 2.0
pad_conductance = 4.0
leakage = 0.05

REACH = 2
PIECES = 4

S0, S1, Q0, Q1, Q2, E0, E1, E2, GUESS = range(9)


def lanes_of(shape):
    return lax.broadcasted_iota(jnp.int32, shape, len(shape) - 1)


def rows_of(shape):
    return lax.broadcasted_iota(jnp.int32, shape, len(shape) - 2)


def pick(record, lane, axis=None):
    kept = jnp.where(lanes_of(record.shape) == lane, record, 0.0)
    return jnp.sum(kept, axis=axis, keepdims=True)


def by_lane(shape, entries):
    lane = lanes_of(shape)
    out = jnp.zeros(shape, jnp.float32)
    for where, value in entries:
        out = jnp.where(lane == where, value, out)
    return out


def fold(value):
    parts = [value[:, i : i + 128] for i in range(0, value.shape[1], 128)]
    while len(parts) > 1:
        parts = [a + b for a, b in zip(parts[::2], parts[1::2])]
    return parts[0]


def kernel(
    nz,
    nx,
    nc,
    cur_hbm,
    cls_hbm,
    cc_hbm,
    pad_hbm,
    via_hbm,
    cur,
    z_p,
    w,
    y_p,
    u,
    scal_ref,
    cc_ref,
    cls,
    pad,
    via,
    cond_p,
    edges,
    coupling,
    base,
    inv,
    zother,
    yother,
    raw_row,
    raw_col,
    raw_corner,
    got_row,
    got_col,
    got_corner,
    y_row,
    y_col,
    goty_row,
    goty_col,
    srec,
    near,
    zrec,
    zbuf,
    in_sem,
    halo_ssem,
    halo_rsem,
    other_ssem,
    other_rsem,
    near_ssem,
    near_rsem,
    z_ssem,
    z_rsem,
    mid_rsem,
    pass_sem,
    low,
    zero_in,
    high,
):
    iz, ix, ic = lax.axis_index("row"), lax.axis_index("col"), lax.axis_index("layer")
    rows, cols = cur.shape
    unroll = 4
    chunks = rows // 8
    reach = REACH
    me = ix * nc + ic

    loads = [
        pltpu.make_async_copy(src, dst, in_sem.at[i])
        for i, (src, dst) in enumerate(
            ((cc_hbm, cc_ref), (cls_hbm, cls), (cur_hbm, cur), (pad_hbm, pad), (via_hbm, via))
        )
    ]
    for copy in loads:
        copy.start()

    for buffer in (got_row, got_col, got_corner, goty_row, goty_col, near, zbuf):
        buffer[...] = jnp.zeros(buffer.shape, jnp.float32)

    def device(dz, dx, dc=0):
        where = {}
        for name, index, size, step in (
            ("row", iz, nz, dz),
            ("col", ix, nx, dx),
            ("layer", ic, nc, dc),
        ):
            if step % size:
                where[name] = lax.rem(index + step % size, size)
        return where

    plane = [(dx, dc) for dx in range(nx) for dc in range(nc)]
    greets = [(0, dx, dc) for dx, dc in plane[1:]]
    greets += [(dz, dx, 0) for dz in (-1, 1) for dx in (0, -1, 1)]
    barrier = pltpu.get_barrier_semaphore()
    for steps in greets:
        pl.semaphore_signal(
            barrier, inc=1, device_id=device(*steps), device_id_type=MESH
        )

    early = max(nz - 5, 2)

    mid_first, mid_stop = max(nz // 4, 2), min(3 * nz // 4, nz - 1 - reach) + 1
    mids = mid_stop - mid_first

    def middle(row):
        return (row >= mid_first) & (row < mid_stop)


    def tell(semaphore, row):
        pl.semaphore_signal(
            semaphore, inc=1, device_id={"row": row}, device_id_type=MESH
        )

    def announce():
        pl.when(iz >= 3)(lambda: pl.semaphore_wait(low, 1))
        pl.when((iz >= 2) & (iz < nz - 1))(lambda: tell(low, iz + 1))

        def one(row, carry):
            tell(high.at[iz], row)
            return carry

        lax.fori_loop(1, iz, one, 0)

    def introduce(row):
        tell(high.at[row], 0)
        pl.when(jnp.logical_not(middle(row)))(lambda: tell(zero_in, row))

    def introduce_early():
        def one(row, carry):
            pl.semaphore_wait(high.at[row], 1)
            introduce(row)
            return carry

        lax.fori_loop(2, early + 1, one, 0)

    def introduce_late():
        pl.semaphore_wait(zero_in, 1)
        tell(high.at[nz - 1], 0)
        for row in range(early + 1, nz - 1):
            introduce(row)

    def meet_all():
        def one(row, carry):
            pl.semaphore_wait(high.at[row], 1)
            return carry

        lax.fori_loop(2, nz, one, 0)

    def meet(row):
        known = jnp.where(iz == 0, nz, jnp.where(iz == 1, early, 0))
        pl.when((row > iz) & (row > known))(lambda: pl.semaphore_wait(high.at[row], 1))
        pl.when((row == 0) & (iz >= 2) & (iz < nz - 1) & jnp.logical_not(middle(iz)))(
            lambda: pl.semaphore_wait(zero_in, 1)
        )

    inside = {
        ("row", -1): iz > 0,
        ("row", 1): iz < nz - 1,
        ("col", -1): ix > 0,
        ("col", 1): ix < nx - 1,
    }

    def exists(dz, dx):
        flags = [inside["row", dz]] if dz else []
        flags += [inside["col", dx]] if dx else []
        return functools.reduce(jnp.logical_and, flags)

    slot = {-1: 0, 1: 1}
    raw = [(dz, 0, raw_row.at[slot[dz]], got_row, slot[-dz]) for dz in (-1, 1)]
    raw += [(0, dx, raw_col.at[slot[dx]], got_col, slot[-dx]) for dx in (-1, 1)]
    raw += [
        (
            dz,
            dx,
            raw_corner.at[2 * slot[dz] + slot[dx]],
            got_corner,
            2 * slot[-dz] + slot[-dx],
        )
        for dz in (-1, 1)
        for dx in (-1, 1)
    ]
    image_halo = [(dz, 0, y_row.at[slot[dz]], goty_row, slot[-dz]) for dz in (-1, 1)]
    image_halo += [(0, dx, y_col.at[slot[dx]], goty_col, slot[-dx]) for dx in (-1, 1)]

    def halo(turn, table, i):
        dz, dx, src, dst, there = table[i]
        return pltpu.make_async_remote_copy(
            src_ref=src,
            dst_ref=dst.at[there],
            send_sem=halo_ssem.at[turn, i],
            recv_sem=halo_rsem.at[turn, i],
            device_id=device(dz, dx),
            device_id_type=MESH,
        )

    def send_halo(turn, table):
        for i, (dz, dx, *_) in enumerate(table):
            pl.when(exists(dz, dx))(halo(turn, table, i).start)

    def take_halo(turn, table):
        for i, (dz, dx, *_) in enumerate(table):
            pl.when(exists(-dz, -dx))(halo(turn, table, i).wait_recv)

    def end_halo(turn, table):
        for i, (dz, dx, *_) in enumerate(table):
            pl.when(exists(dz, dx))(halo(turn, table, i).wait_send)

    pieces = PIECES
    share = rows // pieces

    def to_other(turn, src, dst, piece):
        return pltpu.make_async_remote_copy(
            src_ref=src.at[pl.ds(8 + piece * share, share)],
            dst_ref=dst.at[pl.ds(piece * share, share)],
            send_sem=other_ssem.at[turn, piece],
            recv_sem=other_rsem.at[turn, piece],
            device_id={"layer": 1 - ic},
            device_id_type=MESH,
        )

    def by_piece(body, carry, before=None, after=None):
        for piece in range(pieces):
            if before:
                before(piece)
            first, stop = piece * share // 8, (piece + 1) * share // 8
            carry = lax.fori_loop(first, stop, body, carry, unroll=unroll)
            if after:
                after(piece)
        return carry

    tile = (8, cols)
    block = (8, 128)
    zero = jnp.zeros(block, jnp.float32)
    sub = rows_of(tile)
    narrow_lane = lanes_of(block)

    def at(k, shift=0):
        return pl.ds(pl.multiple_of(8 * k + shift, 8), 8)

    def packed(k, value, left, right):
        here = narrow_lane == k
        left = jnp.where(here, pltpu.roll(value[:, :128], k, 1), left)
        right = jnp.where(here, pltpu.roll(value[:, cols - 128 :], k + 1, 1), right)
        return left, right

    def around(k, prev, here, after, left, right):
        up = pltpu.roll(jnp.where(sub == 7, prev, here), 1, 0)
        down = pltpu.roll(jnp.where(sub == 0, after, here), 7, 0)
        left = pltpu.roll(left, lax.rem(128 - k, 128), 1)
        right = pltpu.roll(right, 127 - k, 1)
        west = pltpu.roll(here, 1, 1)
        west = jnp.concatenate(
            [jnp.where(narrow_lane == 0, left, west[:, :128]), west[:, 128:]], axis=1
        )
        east = pltpu.roll(here, cols - 1, 1)
        east = jnp.concatenate(
            [
                east[:, : cols - 128],
                jnp.where(narrow_lane == 127, right, east[:, cols - 128 :]),
            ],
            axis=1,
        )
        return up, down, west, east

    for copy in loads:
        copy.wait()
    last = cols - 128

    def place(k, value, lane, out):
        moved = pltpu.roll(value, lax.rem(k + 128 - lane, 128), 1)
        return jnp.where(narrow_lane == k, moved, out)

    def node(k, lanes):
        klass = cls[at(k), lanes]
        level = [cc_ref[0, i] for i in range(8)]
        for bit in range(3):
            high_bit = (klass & (1 << bit)) != 0
            level = [jnp.where(high_bit, b, a) for a, b in zip(level[::2], level[1::2])]
        across = via_conductance * via[at(k), lanes].astype(jnp.float32)
        rest = pad_conductance * pad[at(k), lanes].astype(jnp.float32) + leakage
        return level[0], across, across + rest

    def look_up(k, carry):
        cond_p[at(k, 8), :], coupling[at(k), :], base[at(k), :] = node(k, slice(None))
        return carry

    def look_up_ends(k, carry):
        cond, _, rest = node(k, pl.ds(0, 128))
        load = cur[at(k), 0:128]
        borders = [(cond, 0), (cond, 1), (rest, 0), (load, 0)]
        cond, _, rest = node(k, pl.ds(last, 128))
        load = cur[at(k), last:cols]
        borders += [(cond, 127), (cond, 126), (rest, 127), (load, 127)]
        return tuple(place(k, *border, out) for border, out in zip(borders, carry))

    look_up(0, 0)
    look_up(chunks - 1, 0)
    packs = lax.fori_loop(0, chunks, look_up_ends, (zero,) * 8, unroll=8)
    for i in range(8):
        raw_col[i // 4, i % 4] = packs[i]
    for side, row in ((0, 0), (1, rows - 1)):
        inward = 1 - 2 * side
        raw_row[side, 0] = cond_p[8 + row : 9 + row, :]
        raw_row[side, 1] = cond_p[8 + row + inward : 9 + row + inward, :]
        raw_row[side, 2] = base[row : row + 1, :]
        raw_row[side, 3] = cur[row : row + 1, :]
        for end, col in ((0, 0), (1, cols - 1)):
            corner = cond_p[8 + row : 9 + row, col : col + 1]
            raw_corner[2 * side + end] = jnp.broadcast_to(corner, block)

    pl.semaphore_wait(barrier, len(greets))
    send_halo(0, raw)
    announce()
    pl.when(iz == 1)(introduce_early)
    lax.fori_loop(1, chunks - 1, look_up, 0, unroll=unroll)
    take_halo(0, raw)
    pl.when(iz == 0)(lambda: tell(zero_in, nz - 1))
    pl.when(iz == nz - 1)(introduce_late)
    for side, row in ((0, 0), (1, rows + 8)):
        cond_p[row : row + 8, :] = jnp.broadcast_to(got_row[side, 0], tile)

    cond_left, cond_right = got_col[0, 0], got_col[1, 0]

    def edge(here, other):
        return jnp.where(other > 0.0, 0.5 * (here + other), 0.0)

    def precondition(k, energy):
        here = cond_p[at(k, 8), :]
        sides = around(
            k, cond_p[at(k), :], here, cond_p[at(k, 16), :], cond_left, cond_right
        )
        sides = [edge(here, other) for other in sides]
        for i in range(4):
            edges[i, at(k), :] = sides[i]
        diagonal = ((sides[0] + sides[1]) + (sides[2] + sides[3])) + base[at(k), :]
        inverse = 1.0 / diagonal
        resid = cur[at(k), :]
        value = resid * inverse
        inv[at(k), :] = inverse
        z_p[at(k, 8), :] = value
        return energy + fold(resid * value)

    energy = by_piece(
        precondition, zero, after=lambda piece: to_other(0, z_p, zother, piece).start()
    )

    def beyond(here, others, rest, load):
        sides = [edge(here, other) for other in others]
        diagonal = ((sides[0] + sides[1]) + (sides[2] + sides[3])) + rest
        return jnp.where(here > 0.0, load * (1.0 / diagonal), 0.0)

    for side, row, inner in ((0, 0, 8), (1, rows + 8, rows + 7)):
        here, outer, rest, load = [
            jnp.broadcast_to(got_row[side, i], tile) for i in range(4)
        ]
        inner = jnp.broadcast_to(cond_p[inner : inner + 1, :], tile)
        west = pltpu.roll(here, 1, 1)
        west = jnp.concatenate(
            [
                jnp.where(narrow_lane == 0, got_corner[2 * side], west[:, :128]),
                west[:, 128:],
            ],
            axis=1,
        )
        east = pltpu.roll(here, cols - 1, 1)
        east = jnp.concatenate(
            [
                east[:, :last],
                jnp.where(narrow_lane == 127, got_corner[2 * side + 1], east[:, last:]),
            ],
            axis=1,
        )
        z_p[row : row + 8, :] = beyond(here, (outer, inner, west, east), rest, load)

    narrow_sub = rows_of(block)
    z_ends = []
    for side in range(2):
        here, outer, rest, load = [got_col[side, i] for i in range(4)]
        up = pltpu.roll(here, 1, 0)
        up = jnp.where(narrow_sub == 0, pltpu.roll(up, 1, 1), up)
        up = jnp.where((narrow_sub == 0) & (narrow_lane == 0), got_corner[side], up)
        down = pltpu.roll(here, 7, 0)
        down = jnp.where(narrow_sub == 7, pltpu.roll(down, 127, 1), down)
        end = (narrow_sub == 7) & (narrow_lane == chunks - 1)
        down = jnp.where(end, got_corner[2 + side], down)
        inner = raw_col[side, 0]
        z_ends.append(beyond(here, (up, down, outer, inner), rest, load))
    z_left, z_right = z_ends

    def image(k, field, lead, left, right, other):
        values = [field[at(k, 8 * i), :] for i in range(3)]
        sides = around(k, *values, left, right)
        terms = [edges[i, at(k), :] * sides[i] for i in range(4)]
        beside = (terms[0] + terms[1]) + (terms[2] + terms[3])
        return lead - beside - coupling[at(k), :] * other[at(k), :], values[1]

    def first_image(k, carry):
        left, right, curve = carry
        out, value = image(k, z_p, cur[at(k), :], z_left, z_right, zother)
        w[at(k), :] = out
        nxt = out * inv[at(k), :]
        y_p[at(k, 8), :] = nxt
        left, right = packed(k, nxt, left, right)
        return left, right, curve + fold(value * out)

    left, right, curve = by_piece(
        first_image,
        (zero, zero, zero),
        before=lambda piece: to_other(0, z_p, zother, piece).wait_recv(),
        after=lambda piece: to_other(1, y_p, yother, piece).start(),
    )
    y_row[0] = y_p[8:9, :]
    y_row[1] = y_p[rows + 7 : rows + 8, :]
    y_col[0] = left
    y_col[1] = right
    send_halo(1, image_halo)
    energy = jnp.sum(energy, keepdims=True)
    curve = jnp.sum(curve, keepdims=True)
    guess = energy / curve
    pl.when(iz == 0)(meet_all)
    take_halo(1, image_halo)
    for side, row in ((0, 0), (1, rows + 8)):
        y_p[row : row + 8, :] = jnp.broadcast_to(goty_row[side], tile)

    y_left, y_right = goty_col[0], goty_col[1]

    def second_image(k, sums):
        along = w[at(k), :]
        out, nxt = image(k, y_p, along, y_left, y_right, yother)
        u[at(k), :] = out
        left_over = cur[at(k), :] - guess * along
        pre = left_over * inv[at(k), :]
        pre_image = along - guess * out
        terms = (
            left_over * pre,
            left_over * nxt,
            along * nxt,
            pre * pre_image,
            pre * out + nxt * pre_image,
            nxt * out,
        )
        return tuple(a + fold(b) for a, b in zip(sums, terms))

    sums = by_piece(
        second_image,
        (zero,) * 6,
        before=lambda piece: to_other(1, y_p, yother, piece).wait_recv(),
    )

    line = (1, 128)
    entries = [(S0, energy), (S1, curve), (GUESS, guess)]
    entries += [
        (spot, jnp.sum(value, keepdims=True))
        for spot, value in zip((Q0, Q1, Q2, E0, E1, E2), sums)
    ]
    record = by_lane(line, entries)
    srec[...] = record
    near[len(plane) + me] = record

    everyone = range(len(plane))

    def several(ref, first, count, semaphore):
        part = ref.at[pl.ds(first, count)]
        return pltpu.make_async_remote_copy(
            src_ref=part,
            dst_ref=part,
            send_sem=semaphore,
            recv_sem=semaphore,
            device_id=device(1, 0),
            device_id_type=MESH,
        )

    def close(dz, i):
        dx, dc = plane[i]
        where = device(0, dx, dc)
        where["row"] = lax.rem(iz + dz + nz, nz)
        spot = dz + 1
        return pltpu.make_async_remote_copy(
            src_ref=srec,
            dst_ref=near.at[spot * len(plane) + me],
            send_sem=near_ssem.at[spot],
            recv_sem=near_rsem.at[spot],
            device_id=where,
            device_id_type=MESH,
        )

    def close_arrived(spot):
        count = len(plane) - (spot == 1)
        several(near, spot * len(plane), count, near_rsem.at[spot]).wait_recv()

    def greet_plane(dz):
        meet(lax.rem(iz + dz + nz, nz))
        for i in everyone:
            close(dz, i).start()

    def greet_up(dz):
        pl.when(iz + dz >= nz)(lambda: greet_plane(dz))

    def close_left(spot):
        count = len(plane) - (spot == 1)
        several(near, 0, count, near_ssem.at[spot]).wait_send()

    turned = jnp.where(iz >= nz - reach, nz - 1 - iz, 0)
    ups = [1 + lax.rem(i + turned, reach) for i in range(reach)]
    for i in everyone[1:]:
        close(0, i).start()
    for dz in ups:
        greet_up(dz)
    pl.when(iz == 1)(lambda: greet_plane(-1))
    part = pl.ds(mid_first, mids)
    hand_on = pltpu.make_async_remote_copy(
        src_ref=zbuf.at[part],
        dst_ref=zbuf.at[part],
        send_sem=pass_sem,
        recv_sem=mid_rsem,
        device_id={"row": 0},
        device_id_type=MESH,
    )

    def pass_on():
        hand_on.wait_recv()
        hand_on.start()

    pl.when(iz == 1)(pass_on)
    close_arrived(1)

    records = near[pl.ds(len(plane), len(plane))].reshape(len(plane), 128)
    joint = pick(records, S0) / pick(records, S1)
    delta = joint - pick(records, GUESS, axis=1)
    first = by_lane(
        records.shape,
        [(Q0, -2.0 * delta), (Q1, -delta), (E0, -delta), (E1, -2.0 * delta)],
    )
    second = by_lane(records.shape, [(Q0, delta * delta), (E0, delta * delta)])
    records = (
        records
        + first * pltpu.roll(records, 127, 1)
        + second * pltpu.roll(records, 126, 1)
    )
    record = jnp.sum(records, axis=0, keepdims=True)
    record = jnp.where(lanes_of(line) == GUESS, joint, record)
    zrec[...] = record

    def along_z(row, received=z_rsem):
        return pltpu.make_async_remote_copy(
            src_ref=zrec,
            dst_ref=zbuf.at[iz],
            send_sem=z_ssem,
            recv_sem=received,
            device_id={"row": row},
            device_id_type=MESH,
        )

    def direct(source, row):
        near_by = (row + nz - source <= reach) & (row < source)
        return near_by | ((row == 0) & ((source == 1) | middle(source)))

    def far_rows(first, stop, act, leaving=True):
        def one(row, carry):
            pair = (iz, row) if leaving else (row, iz)
            far = (row != iz) & jnp.logical_not(direct(*pair))
            pl.when(far)(lambda: act(row))
            return carry

        lax.fori_loop(first, stop, one, 0)

    def met_send(row):
        meet(row)
        along_z(row).start()

    far_rows(0, jnp.minimum(iz, 1), met_send)
    pl.when(middle(iz))(lambda: along_z(1, mid_rsem).start())
    own = jnp.where(middle(iz), 2, 1)
    far_rows(own, iz, lambda row: along_z(row).start())
    far_rows(iz + 1, nz, met_send)

    end_halo(0, raw)
    end_halo(1, image_halo)
    for piece in range(pieces):
        to_other(0, z_p, zother, piece).wait_send()
        to_other(1, y_p, yother, piece).wait_send()
    close_left(1)
    pl.when(iz == 1)(lambda: close_left(0))
    for step in range(1, reach + 1):
        pl.when(iz + step >= nz)(lambda step=step: close_left(step + 1))

    def wait_far(row, count, receive):
        copies = several(zbuf, 0, count, z_rsem if receive else z_ssem)
        pl.when(row)(copies.wait_recv if receive else copies.wait_send)

    wait_far((iz != 1) & (iz < nz - reach) & jnp.logical_not(middle(iz)), nz - 1, False)
    wait_far(middle(iz), nz - 2, False)
    wait_far(iz == 1, nz - 2, False)
    for step in range(reach):
        wait_far(iz == nz - 1 - step, nz - 1 - reach + step, False)
    wait_far(iz == 0, nz - 2 - reach - mids, True)
    for row in range(1, max(reach, 2)):
        count = nz - 1 - max(reach - row, 0)
        wait_far(iz == row, count - mids * (row == 1), True)
    wait_far(iz >= max(reach, 2), nz - 1, True)
    pl.when(iz == 0)(hand_on.wait_recv)
    pl.when(iz == 1)(hand_on.wait_send)
    pl.when(iz == 0)(lambda: close_arrived(0))
    for step in range(reach, 0, -1):
        pl.when(iz < step)(lambda step=step: close_arrived(step + 1))

    records = [near[...].reshape(near.shape[0], 128), zbuf[...].reshape(nz, 128)]
    records = jnp.concatenate(records, axis=0)
    energy, curve = pick(records, S0), pick(records, S1)
    first_step = energy / curve
    delta = first_step - pick(records, GUESS, axis=1)
    weight = by_lane(records.shape, [(Q0, 1.0), (Q1, -2.0 * delta), (Q2, delta * delta)])
    energy_next = jnp.sum(weight * records, keepdims=True)
    weight = by_lane(records.shape, [(E0, 1.0), (E1, -delta), (E2, delta * delta)])
    curve_next = jnp.sum(weight * records, keepdims=True)
    ratio = energy_next / energy
    second_step = energy_next / (curve_next - ratio * energy_next / first_step)
    both = first_step + second_step * (1.0 + ratio)
    back = first_step * second_step
    for i, value in enumerate((first_step, both, back)):
        scal_ref[i] = jnp.broadcast_to(value, block)


def finish(cur, z_p, w, y_p, u, scal, drop_hbm, resid_hbm, worst_hbm, drop, resid, worst, sem):
    rows, cols = cur.shape
    pieces = 4
    size = rows // pieces
    wide = [jnp.concatenate([scal[i]] * (cols // 128), axis=1) for i in range(3)]
    copies = []
    for piece in range(pieces):
        for k in range(size // 8):
            at = pl.ds(piece * size + 8 * k, 8)
            below = pl.ds(piece * size + 8 * k + 8, 8)
            z = z_p[below, :]
            new = wide[1] * z - wide[2] * y_p[below, :]
            drop[at, :] = new
            resid[at, :] = cur[at, :] - wide[1] * w[at, :] + wide[2] * u[at, :]
            worst[at, :] = jnp.maximum(wide[0] * z, new)
        part = pl.ds(piece * size, size)
        for i, (src, dst) in enumerate(
            ((drop, drop_hbm), (resid, resid_hbm), (worst, worst_hbm))
        ):
            copy = pltpu.make_async_copy(src.at[part], dst.at[part], sem.at[i, piece])
            copy.start()
            copies.append(copy)
    for copy in copies:
        copy.wait()


def local(nz, nx, nc, current, node_class, class_conductance, pad_mask, via_mask):
    rows, cols = via_mask.shape
    field = jax.ShapeDtypeStruct((rows, cols), jnp.float32)
    tall = jax.ShapeDtypeStruct((rows + 16, cols), jnp.float32)
    full = pltpu.VMEM((rows, cols), jnp.float32)
    whole = pltpu.VMEM((rows, cols), jnp.int32)
    padded = pltpu.VMEM((rows + 16, cols), jnp.float32)
    hbm = pl.BlockSpec(memory_space=pltpu.HBM)
    vmem = pl.BlockSpec(memory_space=pltpu.VMEM)
    dma = pltpu.SemaphoreType.DMA
    scratch = [pltpu.SMEM(class_conductance.shape, jnp.float32)]
    scratch += [whole, whole, whole, padded, pltpu.VMEM((4, rows, cols), jnp.float32)]
    scratch += [full] * 5
    near = (REACH + 2) * nx * nc
    scratch += [
        pltpu.VMEM((2, 4, 1, cols), jnp.float32),
        pltpu.VMEM((2, 4, 8, 128), jnp.float32),
        pltpu.VMEM((4, 8, 128), jnp.float32),
    ] * 2
    scratch += [
        pltpu.VMEM((2, 1, cols), jnp.float32),
        pltpu.VMEM((2, 8, 128), jnp.float32),
    ] * 2
    scratch += [
        pltpu.VMEM((1, 128), jnp.float32),
        pltpu.VMEM((near, 1, 128), jnp.float32),
        pltpu.VMEM((1, 128), jnp.float32),
        pltpu.VMEM((nz, 1, 128), jnp.float32),
        dma((5,)),
        dma((2, 8)),
        dma((2, 8)),
        dma((2, PIECES)),
        dma((2, PIECES)),
        dma((REACH + 2,)),
        dma((REACH + 2,)),
        dma,
        dma,
        dma,
        dma,
        pltpu.SemaphoreType.REGULAR,
        pltpu.SemaphoreType.REGULAR,
        pltpu.SemaphoreType.REGULAR((nz,)),
    ]
    limit = 32 * 1024 * 1024
    scalars = jax.ShapeDtypeStruct((3, 8, 128), jnp.float32)
    args = (current[0], node_class[0], class_conductance, pad_mask[0], via_mask)
    stay = [pltpu.with_memory_space_constraint(arg, pltpu.HBM) for arg in args]
    solved = pl.pallas_call(
        functools.partial(kernel, nz, nx, nc),
        out_shape=[field, tall, field, tall, field, scalars],
        in_specs=[hbm] * 5,
        out_specs=[vmem] * 6,
        scratch_shapes=scratch,
        compiler_params=pltpu.CompilerParams(
            collective_id=0, has_side_effects=True, vmem_limit_bytes=limit
        ),
    )(*stay)
    outs = pl.pallas_call(
        finish,
        out_shape=[field] * 3,
        in_specs=[vmem] * 6,
        out_specs=[hbm] * 3,
        scratch_shapes=[full] * 3 + [dma((3, 4))],
        compiler_params=pltpu.CompilerParams(vmem_limit_bytes=limit),
    )(*solved)
    return tuple(out[None] for out in outs)


def solution(mesh):
    grid = P("layer", ("scen", "row"), "col")
    in_specs = (grid, grid, P("layer", None), grid, P(("scen", "row"), "col"))
    sizes = (mesh.shape["row"], mesh.shape["col"], mesh.shape["layer"])
    return jax.shard_map(
        functools.partial(local, *sizes),
        mesh=mesh,
        in_specs=in_specs,
        out_specs=(grid, grid, grid),
        check_vma=False,
    )
```
